32 devices in a mesh: gx: 16 (over z, y, x), gy: 2 (over core).
Axes of the slice: x: 2, y: 2, z: 4, core: 2. Of those that a mesh axis runs over, the one named last changes fastest.
Arguments:
- sources: bfloat16 [2048, 8, 128], P(('gx', 'gy')), may hold values from -6 to 6
- owners: int32 [2048, 1], P(('gx', 'gy')), may hold values from 0 to 15; in each aligned block of 64 rows (0 to 63, 64 to 127, ...) at most 8 rows name the same one
- strip_rows: int32 [2048], P(('gx', 'gy')), may hold values from 0 to 255
- panel_counts: int32 [2048], P(('gx', 'gy')), may hold values from 1 to 128
- arrival_bins: int32 [4096, 4, 128], P('gx'), may hold values from 0 to 254
- arrival_fracs: float32 [4096, 4, 128], P('gx'), may hold values from 0 to 1
- gain_table: bfloat16 [4096, 8, 4, 1024], P('gx'), may hold values from -0.125 to 0.125
Outputs:
- signals: float32 [1024, 4, 256], P(('gx', 'gy'))
The draws below stay inside these ranges and needn't reach their ends.
Inputs may be any that keep to these rules, and one draw needn't show every extreme that they name: `owners`: among the rows of one device, at most 8 strips name one patch, a bound that some block reaches.
All inputs are finite; a program needn't handle non-finite values.
Results may differ from the reference program's by a relative error of at most 0.0044.
Values may be sent and summed in bfloat16 or wider, within the bound.
A program may use at most 768 MiB of HBM per device.

```python
import math
import jax
import jax.numpy as jnp
import numpy as np
from jax import lax

TERMS = 8
SP = 128
NBIN = 256
NOB = 4
OBS_BLOCK = 1024
STRIP_DEV = 64
ROWS = 256
CAP = 8
STRIPS = 2048
TROWS = 4096
N_GX = 16


def set_ends(array, stream_key, low, high):
    longest = array.shape.index(max(array.shape))
    spots = []
    for shift in (0, 1):
        where = [jax.random.randint(jax.random.fold_in(stream_key, axis), (), 0, length) for axis, length in enumerate(array.shape)]
        where[longest] = (where[longest] + shift) % array.shape[longest]
        spots.append(tuple(where))
    return array.at[spots[0]].set(low).at[spots[1]].set(high)


def spiked(drawn, key, source, target, shards_of, factor):
    owner, partner = [(jnp.arange(drawn.shape[axis_at]) // (drawn.shape[axis_at] // shards_of)).reshape([-1 if axis == axis_at else 1 for axis in range(drawn.ndim)]) for axis_at in (source, target)]
    chosen = jax.random.permutation(key, shards_of)[partner]
    strong = (owner == chosen) | (owner == (partner + shards_of // 2) % shards_of)
    return jnp.where(strong, factor * drawn, drawn)


def level_of(own_key, shape, pieces, low, largest):
    def one(position, parts):
        heights = jax.random.uniform(jax.random.fold_in(jax.random.fold_in(own_key, 6), position), (parts,), jnp.float32, low / len(pieces), largest / len(pieces))
        return jnp.repeat(jnp.exp(heights), shape[position] // parts).reshape((-1,) + (1,) * (len(shape) - position - 1))

    level = one(*pieces[0])
    for cut in pieces[1:]:
        level = level * one(*cut)
    return level


def assign_block(key, own, number, rows, count, top, most, slope):
    order = jax.random.permutation(key, count)
    crowded, usual = portions_of(count, rows * top, most, slope, True), portions_of(count, rows * top, most, slope, False)
    places = jnp.arange(count)

    def named(sizes, turn):
        used = int((sizes > 0).sum())
        fixed = max(1, used // 4)
        passed = fixed + (places - fixed + turn * (used - fixed)) % max(1, count - fixed)
        return jnp.zeros((count,), jnp.int32).at[order[jnp.where(places < fixed, places, passed)]].set(jnp.asarray(sizes, jnp.int32))

    sizes = jnp.where(number % 4 == 0, named(crowded, number // 4), named(usual, number - number // 4 - 1))
    mixed = jax.random.permutation(jax.random.fold_in(own, 3), count)
    donor, receiver = mixed[0:count // 2 * 2:2], mixed[1:count // 2 * 2:2]
    slack = jnp.minimum(sizes[donor] - 1, most - sizes[receiver]) // 2
    slack = jnp.where((donor == order[0]) | (receiver == order[0]) | (sizes[receiver] == 0), 0, jnp.maximum(slack, 0))
    passed = jax.random.randint(jax.random.fold_in(own, 4), (count // 2,), 0, 1 << 20) % (slack + 1)
    sizes = sizes.at[donor].add(-passed).at[receiver].add(passed)
    members = jnp.searchsorted(jnp.cumsum(sizes), jnp.arange(rows * top), side="right").astype(jnp.int32)
    listing = members.reshape(top, rows).T
    listing = listing[jax.random.permutation(jax.random.fold_in(own, 1), rows)]
    turn = jax.random.randint(jax.random.fold_in(own, 2), (rows, 1), 0, top)
    return jnp.take_along_axis(listing, (jnp.arange(top)[None, :] + turn) % top, axis=1)


def portions_of(count, total, reach, slope, full):
    loads = [(1 << 20) // math.isqrt(standing ** slope) + 1 for standing in range(1, count + 1)]
    largest = reach if full else min(reach, max(-(-total // count), total * loads[0] // sum(loads)))
    least = 1 if total - largest >= count - 1 else 0
    holding, surplus = [largest] + [least] * (count - 1), total - largest - least * (count - 1)
    while surplus > 0:
        free = [i for i in range(1, count) if holding[i] < largest] or [i for i in range(1, count) if holding[i] < reach]
        pool, budget = sum([loads[i] for i in free]), surplus
        for i in free:
            more = min(reach - holding[i], max(1, budget * loads[i] // pool), surplus)
            holding[i] = holding[i] + more
            surplus = surplus - more
    return np.array(holding)


def gaussian(rng, dims, spread, most, shards=(), held_as=jnp.bfloat16):
    values = spread * jax.random.normal(rng, dims, jnp.float32)
    if shards:
        values = values * level_of(rng, dims, shards, -0.22, 0.18)
    return jnp.clip(values, -most, most).astype(held_as)


def bell_draw_with(key, shape, width, limit, split, heavy, kind=jnp.bfloat16):
    result = width * jax.random.normal(key, shape, jnp.float32)
    if split:
        result = result * level_of(key, shape, split, -0.22, 0.18)
    return jnp.clip(spiked(result, jax.random.fold_in(key, 3), *heavy), -limit, limit).astype(kind)


def setup_inputs(seed: int = 0) -> dict:
    arg_keys = jax.random.split(jax.random.key(seed), 8)
    sources = gaussian(arg_keys[0], (STRIPS, TERMS, SP), 1.0, 6.0, ((0, 32),))
    owners_keys = jax.random.split(jax.random.fold_in(arg_keys[1], 1), STRIPS // STRIP_DEV)
    owners_turns = jax.random.permutation(jax.random.fold_in(arg_keys[1], 3), STRIPS // STRIP_DEV)
    owners = jax.vmap(lambda own, number: assign_block(jax.random.fold_in(arg_keys[1], 2), own, number, STRIP_DEV, N_GX, 1, CAP, 2))(owners_keys, owners_turns).reshape((STRIPS, 1))
    strip_rows = set_ends(jax.random.randint(arg_keys[2], (STRIPS,), 0, ROWS), jax.random.fold_in(arg_keys[2], 1), 0, ROWS - 1).astype(jnp.int32)
    panel_counts = set_ends(jax.random.randint(arg_keys[3], (STRIPS,), 1, SP + 1), jax.random.fold_in(arg_keys[3], 1), 1, SP).astype(jnp.int32)
    arrival_bins = set_ends(jax.random.randint(arg_keys[4], (TROWS, NOB, SP), 0, NBIN - 1), jax.random.fold_in(arg_keys[4], 1), 0, (NBIN - 1) - 1).astype(jnp.int32)
    arrival_fracs = jnp.clip(1.0 * jax.random.uniform(arg_keys[5], (TROWS, NOB, SP), jnp.float32) ** level_of(arg_keys[5], (TROWS, NOB, SP), ((0, 16),), -0.2, 0.2), 0.0, 1.0)
    gain_table = bell_draw_with(arg_keys[6], (TROWS, TERMS, NOB, OBS_BLOCK), TROWS ** -0.5, 0.125, ((0, 16),), (0, 3, 16, 2.0))
    return {"sources": sources, "owners": owners, "strip_rows": strip_rows, "panel_counts": panel_counts, "arrival_bins": arrival_bins, "arrival_fracs": arrival_fracs, "gain_table": gain_table}


def interp_weights(bin_ids, fractions):
    positions = jnp.arange(NBIN, dtype=jnp.int32)
    lower = jnp.where(positions[None, None, :] == bin_ids[:, :, None], 1.0 - fractions[:, :, None], 0.0)
    upper = jnp.where(positions[None, None, :] == bin_ids[:, :, None] + 1, fractions[:, :, None], 0.0)
    return (lower + upper).astype(jnp.bfloat16)


def reference(sources, owners, strip_rows, panel_counts, arrival_bins, arrival_fracs, gain_table):
    live_mask = (jnp.arange(SP, dtype=jnp.int32)[None, :] < panel_counts[:, None]).astype(jnp.float32)
    masked = sources.astype(jnp.float32) * live_mask[:, None, :]
    global_rows = (owners[:, 0] * ROWS + strip_rows).astype(jnp.int32)
    row_sources = jax.ops.segment_sum(masked, global_rows, num_segments=ROWS * N_GX)
    row_rounded = row_sources.astype(jnp.bfloat16)

    def patch_term(running, patch_index):
        first_row = (patch_index * ROWS).astype(jnp.int32)
        patch_sources = lax.dynamic_slice_in_dim(row_rounded, first_row, ROWS, 0).astype(jnp.float32)
        patch_bins = lax.dynamic_slice_in_dim(arrival_bins, first_row, ROWS, 0)
        patch_fracs = lax.dynamic_slice_in_dim(arrival_fracs, first_row, ROWS, 0)
        patch_gains = lax.dynamic_slice_in_dim(gain_table, first_row, ROWS, 0).astype(jnp.float32)
        for block_index in range(NOB):
            weights = interp_weights(patch_bins[:, block_index, :], patch_fracs[:, block_index, :]).astype(jnp.float32)
            arrived = jnp.einsum('rkp,rpb->rkb', patch_sources, weights, precision=lax.Precision.HIGHEST)
            arrived_rounded = arrived.astype(jnp.bfloat16).astype(jnp.float32)
            added = jnp.einsum('rkt,rkb->tb', patch_gains[:, :, block_index, :], arrived_rounded, precision=lax.Precision.HIGHEST)
            running = running.at[:, block_index, :].add(added)
        return running, None

    start_value = jnp.zeros((OBS_BLOCK, NOB, NBIN), jnp.float32)
    signals, unused = lax.scan(patch_term, start_value, jnp.arange(N_GX, dtype=jnp.int32))
    return signals
```

```python
import functools

import jax
import jax.numpy as jnp
from jax import lax
from jax.experimental import pallas as pl
from jax.experimental.pallas import tpu as pltpu
from jax.sharding import PartitionSpec as P

NBIN = 256
LANES = 128
LO = 64
HI = NBIN // LO
WIDE = LO + 16
CHUNK = 128
SLOTS = 4


def bf16(v):
    return v.astype(jnp.bfloat16)


def aligned(i, n):
    return pl.multiple_of(i * n, n)


def gains_kernel(per, blocks, gains_ref, out_ref, buffer, mixed, sems):
    first = lax.axis_index("gy") * per
    columns = out_ref.shape[1] // LANES
    deep = columns * blocks
    group = 256 // deep
    steps = out_ref.shape[2] // CHUNK
    size = CHUNK * deep

    def fetch(i):
        slot = lax.rem(i, SLOTS)
        return pltpu.make_async_copy(
            gains_ref.at[pl.ds(aligned(i, size), size)], buffer.at[slot], sems.at[slot]
        )

    for i in range(SLOTS - 1):
        fetch(i).start()
    height = per * columns * group
    row = lax.broadcasted_iota(jnp.int32, (height, 256), 0)
    spot = lax.broadcasted_iota(jnp.int32, (height, 256), 1)
    wanted = (
        lax.rem(row, group) * deep
        + lax.rem(row // group, columns) * blocks
        + first
        + row // (group * columns)
    )
    pick = bf16((wanted == spot).astype(jnp.float32))

    def step(i, carry):
        slot = lax.rem(i, SLOTS)

        @pl.when(i + SLOTS - 1 < steps)
        def _():
            fetch(i + SLOTS - 1).start()

        fetch(i).wait()

        def part(j, c):
            one = buffer[slot, pl.ds(aligned(j, 512), 256), :]
            two = buffer[slot, pl.ds(aligned(j, 512) + 256, 256), :]
            got = jnp.dot(
                pick, jnp.concatenate([one, two], axis=1), preferred_element_type=jnp.float32
            )
            for o in range(per):
                for t in range(columns):
                    q = (o * columns + t) * group
                    both = jnp.concatenate(
                        [got[q : q + group, :LANES], got[q : q + group, LANES:]], axis=0
                    )
                    mixed[o, pl.ds(aligned(j, 2 * group), 2 * group), t * LANES : (t + 1) * LANES] = bf16(both)
            return c

        lax.fori_loop(0, CHUNK // (2 * group), part, 0, unroll=True)
        for o in range(per):
            for t in range(columns):
                out_ref[o, t * LANES : (t + 1) * LANES, pl.ds(aligned(i, CHUNK), CHUNK)] = mixed[
                    o, :, t * LANES : (t + 1) * LANES
                ].T
        return carry

    lax.fori_loop(0, steps, step, 0)


def turned_gains(per, gain_table):
    rows, terms, blocks, observers = gain_table.shape
    columns = observers // LANES
    flat = (
        gain_table.reshape(rows * terms, blocks, columns, LANES)
        .transpose(0, 2, 1, 3)
        .reshape(-1, LANES)
    )
    return pl.pallas_call(
        functools.partial(gains_kernel, per, blocks),
        out_shape=jax.ShapeDtypeStruct((per, observers, rows * terms), jnp.bfloat16),
        in_specs=[pl.BlockSpec(memory_space=pl.ANY)],
        out_specs=pl.BlockSpec(memory_space=pltpu.VMEM),
        scratch_shapes=[
            pltpu.VMEM((SLOTS, CHUNK * columns * blocks, LANES), jnp.bfloat16),
            pltpu.VMEM((per, CHUNK, observers), jnp.bfloat16),
            pltpu.SemaphoreType.DMA((SLOTS,)),
        ],
        name="turned_gains",
        cost_estimate=pl.CostEstimate(
            flops=4 * 10**9, bytes_accessed=2 * gain_table.size * 2, transcendentals=0
        ),
    )(flat)


def spread_kernel(order, src_ref, bins_ref, fracs_ref, gains_ref, out_ref, table, arrived):
    block = lax.axis_index("gy") * gains_ref.shape[0] + order
    rows = bins_ref.shape[0]
    bins = bins_ref[:, pl.ds(block, 1), :].reshape(rows, LANES)
    fracs = fracs_ref[:, pl.ds(block, 1), :].reshape(rows, LANES)
    table[0] = (bins // LO).astype(jnp.float32)
    table[1] = lax.rem(bins, LO).astype(jnp.float32)
    table[2] = 1.0 - fracs
    table[3] = fracs
    spots = bf16(lax.broadcasted_iota(jnp.int32, (WIDE, LANES), 0).astype(jnp.float32))
    lane = lax.broadcasted_iota(jnp.int32, (16, LANES), 1)
    upper = lax.broadcasted_iota(jnp.int32, (16, LANES), 0) < 8
    zero = jnp.zeros((), jnp.bfloat16)

    def spread(kind, row, n):
        return jnp.broadcast_to(table[kind, pl.ds(row, 1), :], (n, LANES))

    def weights_of(row):
        low = spread(1, row, WIDE)
        return jnp.where(
            spots == bf16(low),
            bf16(spread(2, row, WIDE)),
            jnp.where(spots == bf16(low + 1.0), bf16(spread(3, row, WIDE)), zero),
        )

    def pair(i, carry):
        both = src_ref[pl.ds(aligned(i, 16), 16), :]
        left = bf16(jnp.where(upper, spread(0, 2 * i, 16), -1.0))
        right = bf16(jnp.where(upper, -1.0, spread(0, 2 * i + 1, 16)))
        lhs = []
        for h in range(HI):
            at = jnp.asarray(h, jnp.bfloat16)
            lhs.append(
                jnp.concatenate(
                    [jnp.where(left == at, both, zero), jnp.where(right == at, both, zero)], axis=1
                )
            )
        rhs = jnp.concatenate([weights_of(2 * i), weights_of(2 * i + 1)], axis=1)
        got = lax.dot_general(
            jnp.concatenate(lhs, axis=0), rhs, (((1,), (1,)), ((), ())), preferred_element_type=jnp.float32
        )
        got = jnp.concatenate([got, jnp.zeros((16 * HI, LANES - WIDE), jnp.float32)], axis=1)
        tiles = []
        carried = None
        for t in range(NBIN // LANES):
            even = got[32 * t : 32 * t + 16, :]
            odd = pltpu.roll(got[32 * t + 16 : 32 * t + 32, :], LO, 1)
            tile = even + jnp.where(lane >= LO, odd, 0.0)
            if carried is not None:
                tile = tile + jnp.where(lane < LO, carried, 0.0)
            carried = odd
            tiles.append(tile)
        arrived[pl.ds(aligned(i, 16), 16), :] = bf16(jnp.concatenate(tiles, axis=1))
        return carry

    lax.fori_loop(0, rows // 2, pair, 0, unroll=16)
    tall = 256

    def strip(i, carry):
        out_ref[pl.ds(aligned(i, tall), tall), :] = bf16(
            jnp.dot(
                gains_ref[order, pl.ds(aligned(i, tall), tall), :], arrived[...], preferred_element_type=jnp.float32
            )
        )
        return carry

    lax.fori_loop(0, out_ref.shape[0] // tall, strip, 0)


def partial_signals(order, src, bins, fracs, gains):
    observers = gains.shape[1]
    rows = src.shape[0]
    return pl.pallas_call(
        functools.partial(spread_kernel, order),
        out_shape=jax.ShapeDtypeStruct((observers, NBIN), jnp.bfloat16),
        in_specs=[pl.BlockSpec(memory_space=pltpu.VMEM)] * 4,
        out_specs=pl.BlockSpec(memory_space=pltpu.VMEM),
        scratch_shapes=[
            pltpu.VMEM((4, bins.shape[0], LANES), jnp.float32),
            pltpu.VMEM((rows, NBIN), jnp.bfloat16),
        ],
        name="partial_signals",
        cost_estimate=pl.CostEstimate(
            flops=4 * rows * observers * NBIN, bytes_accessed=8 * 10**6, transcendentals=0
        ),
    )(src, bins, fracs, gains)


def on_device(sources, owners, strip_rows, panel_counts, arrival_bins, arrival_fracs, gain_table):
    strip_count, terms, panels = sources.shape
    shards = lax.axis_size("gx")
    columns = lax.axis_size("gy")
    capacity = 2 * strip_count // shards
    blocks = arrival_bins.shape[1]
    observers = gain_table.shape[3]
    rows_here = arrival_bins.shape[0]
    live_mask = (jnp.arange(panels, dtype=jnp.int32)[None, :] < panel_counts[:, None]).astype(
        jnp.bfloat16
    )
    masked = (sources * live_mask[:, None, :]).reshape(strip_count, terms * panels)
    lane = jnp.arange(128, dtype=jnp.int32)[None, :]
    coded = jnp.where(
        lane == 0,
        (strip_rows // 128)[:, None],
        jnp.where(lane == 1, (strip_rows % 128)[:, None], jnp.where(lane == 2, 1, 0)),
    ).astype(jnp.bfloat16)
    payload = jnp.concatenate([masked, coded], axis=1)
    targets = owners[:, 0]
    earlier = (
        jnp.arange(strip_count, dtype=jnp.int32)[None, :]
        < jnp.arange(strip_count, dtype=jnp.int32)[:, None]
    )
    order_in = jnp.sum(
        jnp.where(earlier & (targets[None, :] == targets[:, None]), 1, 0).astype(jnp.int32), axis=1
    )
    slot_of = targets * capacity + order_in
    placing = jnp.arange(shards * capacity, dtype=jnp.int32)[:, None] == slot_of[None, :]
    send = jnp.dot(
        placing.astype(jnp.bfloat16), payload, preferred_element_type=jnp.float32
    ).astype(jnp.bfloat16)
    got = lax.all_to_all(send, "gx", split_axis=0, concat_axis=0, tiled=True)
    got = lax.all_gather(got, "gy", axis=0, tiled=True)
    codes = got[:, terms * panels :].astype(jnp.int32)
    got_rows = jnp.where(codes[:, 2] > 0, codes[:, 0] * 128 + codes[:, 1], -1)
    row_hot = (jnp.arange(rows_here, dtype=jnp.int32)[:, None] == got_rows[None, :]).astype(
        jnp.bfloat16
    )
    row_sources = jnp.dot(
        row_hot, got[:, : terms * panels], preferred_element_type=jnp.float32
    ).astype(jnp.bfloat16)
    src = row_sources.reshape(rows_here * terms, panels)
    per = blocks // columns
    gains = turned_gains(per, gain_table)
    sums = []
    share = observers // (shards * columns)
    for o in range(per):
        partial = partial_signals(o, src, arrival_bins, arrival_fracs, gains)
        parts = lax.all_to_all(partial, ("gx", "gy"), split_axis=0, concat_axis=0, tiled=True)
        sums.append(
            jnp.sum(parts.reshape(shards, columns, share, NBIN).astype(jnp.float32), axis=0)
        )
    return jnp.stack(sums, axis=1).transpose(2, 0, 1, 3).reshape(share, blocks, NBIN)


def solution(mesh):
    placed = (
        P(("gx", "gy"), None, None),
        P(("gx", "gy"), None),
        P(("gx", "gy")),
        P(("gx", "gy")),
        P("gx", None, None),
        P("gx", None, None),
        P("gx", None, None, None),
    )
    return jax.shard_map(
        on_device,
        mesh=mesh,
        in_specs=placed,
        out_specs=P(("gx", "gy"), None, None),
        check_vma=False,
    )
```

```python
import functools

import jax
import jax.numpy as jnp
from jax import lax
from jax.experimental import pallas as pl
from jax.experimental.pallas import tpu as pltpu
from jax.sharding import PartitionSpec as P

NBIN = 256
LANES = 128
LO = 64
HI = NBIN // LO
WIDE = LO + 16
CHUNK = 128
SLOTS = 4
UNROLL = 16
MESH = pl.DeviceIdType.MESH


def bf16(v):
    return v.astype(jnp.bfloat16)


def aligned(i, n):
    return pl.multiple_of(i * n, n)


def gains_kernel(per, blocks, gains_ref, out_ref, buffer, mixed, sems):
    first = lax.axis_index("gy") * per
    columns = out_ref.shape[1] // LANES
    deep = columns * blocks
    group = 256 // deep
    steps = out_ref.shape[2] // CHUNK
    size = CHUNK * deep

    def fetch(i):
        slot = lax.rem(i, SLOTS)
        return pltpu.make_async_copy(
            gains_ref.at[pl.ds(aligned(i, size), size)], buffer.at[slot], sems.at[slot]
        )

    for i in range(SLOTS - 1):
        fetch(i).start()
    height = per * columns * group
    row = lax.broadcasted_iota(jnp.int32, (height, 256), 0)
    spot = lax.broadcasted_iota(jnp.int32, (height, 256), 1)
    wanted = (
        lax.rem(row, group) * deep
        + lax.rem(row // group, columns) * blocks
        + first
        + row // (group * columns)
    )
    pick = bf16((wanted == spot).astype(jnp.float32))

    def step(i, carry):
        slot = lax.rem(i, SLOTS)

        @pl.when(i + SLOTS - 1 < steps)
        def _():
            fetch(i + SLOTS - 1).start()

        fetch(i).wait()

        def part(j, c):
            one = buffer[slot, pl.ds(aligned(j, 512), 256), :]
            two = buffer[slot, pl.ds(aligned(j, 512) + 256, 256), :]
            got = jnp.dot(
                pick, jnp.concatenate([one, two], axis=1), preferred_element_type=jnp.float32
            )
            for o in range(per):
                for t in range(columns):
                    q = (o * columns + t) * group
                    both = jnp.concatenate(
                        [got[q : q + group, :LANES], got[q : q + group, LANES:]], axis=0
                    )
                    mixed[o, pl.ds(aligned(j, 2 * group), 2 * group), t * LANES : (t + 1) * LANES] = bf16(both)
            return c

        lax.fori_loop(0, CHUNK // (2 * group), part, 0, unroll=True)
        for o in range(per):
            for t in range(columns):
                out_ref[o, t * LANES : (t + 1) * LANES, pl.ds(aligned(i, CHUNK), CHUNK)] = mixed[
                    o, :, t * LANES : (t + 1) * LANES
                ].T
        return carry

    lax.fori_loop(0, steps, step, 0)


def turned_gains(per, gain_table):
    rows, terms, blocks, observers = gain_table.shape
    columns = observers // LANES
    flat = (
        gain_table.reshape(rows * terms, blocks, columns, LANES)
        .transpose(0, 2, 1, 3)
        .reshape(-1, LANES)
    )
    return pl.pallas_call(
        functools.partial(gains_kernel, per, blocks),
        out_shape=jax.ShapeDtypeStruct((per, observers, rows * terms), jnp.bfloat16),
        in_specs=[pl.BlockSpec(memory_space=pl.ANY)],
        out_specs=pl.BlockSpec(memory_space=pltpu.VMEM),
        scratch_shapes=[
            pltpu.VMEM((SLOTS, CHUNK * columns * blocks, LANES), jnp.bfloat16),
            pltpu.VMEM((per, CHUNK, observers), jnp.bfloat16),
            pltpu.SemaphoreType.DMA((SLOTS,)),
        ],
        name="turned_gains",
        cost_estimate=pl.CostEstimate(
            flops=4 * 10**9, bytes_accessed=2 * gain_table.size * 2, transcendentals=0
        ),
    )(flat)


def spread_kernel(
    per, share, src_ref, bins_ref, fracs_ref, gains_hbm, out_ref,
    gains, table, arrived, first_out, first_in, kept, last, second_out, second_in, third_out, third_in,
    gain_sems, one_send, one_recv, two_send, two_recv, three_send, three_recv,
):
    g = lax.axis_index("gx")
    q = lax.axis_index("gy")
    shards = lax.axis_size("gx")
    columns = lax.axis_size("gy")
    depth = shards // 4
    bit0, bit1, z = lax.rem(g, 2), lax.rem(g // 2, 2), g // 4
    flips = (g + 1 - 2 * bit0, g + 2 - 4 * bit1)
    corner = lax.rem(g, 4)
    rows = bins_ref.shape[0]
    wide = columns * share
    tall = depth * wide
    half = NBIN // 2

    def fetch(j):
        return pltpu.make_async_copy(gains_hbm.at[j], gains.at[j], gain_sems.at[j])

    for j in range(per):
        fetch(j).start()

    barrier = pltpu.get_barrier_semaphore()

    def greet(to_g, to_q):
        pl.semaphore_signal(barrier, inc=1, device_id=(to_g, to_q), device_id_type=MESH)

    for partner in flips:
        greet(partner, q)

    def others(body):
        def one(i, c):
            to_z, to_q = i // columns, lax.rem(i, columns)

            @pl.when(jnp.logical_or(to_z != z, to_q != q))
            def _():
                body(i, to_z, to_q)

            return c

        lax.fori_loop(0, depth * columns, one, 0)

    others(lambda i, to_z, to_q: greet(to_z * 4 + corner, to_q))

    spots = bf16(lax.broadcasted_iota(jnp.int32, (WIDE, LANES), 0).astype(jnp.float32))
    lane = lax.broadcasted_iota(jnp.int32, (16, LANES), 1)
    upper = lax.broadcasted_iota(jnp.int32, (16, LANES), 0) < 8
    zero = jnp.zeros((), jnp.bfloat16)

    def prepare(j):
        block = q * per + j
        bins = bins_ref[:, pl.ds(block, 1), :].reshape(rows, LANES)
        fracs = fracs_ref[:, pl.ds(block, 1), :].reshape(rows, LANES)
        table[j, 0] = (bins // LO).astype(jnp.float32)
        table[j, 1] = lax.rem(bins, LO).astype(jnp.float32)
        table[j, 2] = 1.0 - fracs
        table[j, 3] = fracs

    def scatter(j):
        def spread(kind, row, n):
            return jnp.broadcast_to(table[j, kind, pl.ds(row, 1), :], (n, LANES))

        def weights_of(row):
            low = spread(1, row, WIDE)
            return jnp.where(
                spots == bf16(low),
                bf16(spread(2, row, WIDE)),
                jnp.where(spots == bf16(low + 1.0), bf16(spread(3, row, WIDE)), zero),
            )

        def pair(i, carry):
            both = src_ref[pl.ds(aligned(i, 16), 16), :]
            left = bf16(jnp.where(upper, spread(0, 2 * i, 16), -1.0))
            right = bf16(jnp.where(upper, -1.0, spread(0, 2 * i + 1, 16)))
            lhs = []
            for h in range(HI):
                at = jnp.asarray(h, jnp.bfloat16)
                lhs.append(
                    jnp.concatenate(
                        [jnp.where(left == at, both, zero), jnp.where(right == at, both, zero)], axis=1
                    )
                )
            rhs = jnp.concatenate([weights_of(2 * i), weights_of(2 * i + 1)], axis=1)
            got = lax.dot_general(
                jnp.concatenate(lhs, axis=0), rhs, (((1,), (1,)), ((), ())), preferred_element_type=jnp.float32
            )
            got = jnp.concatenate([got, jnp.zeros((16 * HI, LANES - WIDE), jnp.float32)], axis=1)
            tiles = []
            carried = None
            for t in range(NBIN // LANES):
                even = got[32 * t : 32 * t + 16, :]
                odd = pltpu.roll(got[32 * t + 16 : 32 * t + 32, :], LO, 1)
                tile = even + jnp.where(lane >= LO, odd, 0.0)
                if carried is not None:
                    tile = tile + jnp.where(lane < LO, carried, 0.0)
                carried = odd
                tiles.append(tile)
            arrived[pl.ds(aligned(i, 16), 16), :] = bf16(jnp.concatenate(tiles, axis=1))
            return carry

        lax.fori_loop(0, rows // 2, pair, 0, unroll=UNROLL)

    def multiply(j, c0, c1):
        lhs = jnp.concatenate(
            [
                gains[j, pl.ds(pl.multiple_of((k * 4 + c1 * 2 + c0) * wide, 8), wide), :]
                for k in range(depth)
            ],
            axis=0,
        )
        return jnp.dot(lhs, arrived[...], preferred_element_type=jnp.float32)

    def stage_one(j, h, part):
        return pltpu.make_async_remote_copy(
            src_ref=first_out.at[j, h, part],
            dst_ref=first_in.at[j, h, part],
            send_sem=one_send.at[j, h, part],
            recv_sem=one_recv.at[j, h, part],
            device_id=(flips[h], q),
            device_id_type=MESH,
        )

    def stage_two(j, h):
        return pltpu.make_async_remote_copy(
            src_ref=second_out.at[j, h],
            dst_ref=second_in.at[j, h],
            send_sem=two_send.at[j, h],
            recv_sem=two_recv.at[j, h],
            device_id=(flips[1 - h], q),
            device_id_type=MESH,
        )

    def stage_three(j, i, to_z, to_q):
        return pltpu.make_async_remote_copy(
            src_ref=third_out.at[j, i],
            dst_ref=third_in.at[j, z * columns + q],
            send_sem=three_send.at[j, i],
            recv_sem=three_recv.at[j, z * columns + q],
            device_id=(to_z * 4 + corner, to_q),
            device_id_type=MESH,
        )

    def arrival(j, i):
        return pltpu.make_async_remote_copy(
            src_ref=third_out.at[j, i],
            dst_ref=third_in.at[j, i],
            send_sem=three_send.at[j, i],
            recv_sem=three_recv.at[j, i],
            device_id=((i // columns) * 4 + corner, lax.rem(i, columns)),
            device_id_type=MESH,
        )

    sides = (slice(0, half), slice(half, NBIN))

    def products(j):
        got = multiply(j, 1 - bit0, 1 - bit1)
        for h in range(2):
            first_out[j, h, 0] = bf16(got[:, sides[h]])
            stage_one(j, h, 0).start()
        got = multiply(j, 1 - bit0, bit1)
        first_out[j, 0, 1] = bf16(got[:, sides[0]])
        stage_one(j, 0, 1).start()
        kept[j, 1] = got[:, sides[1]]
        got = multiply(j, bit0, 1 - bit1)
        first_out[j, 1, 1] = bf16(got[:, sides[1]])
        stage_one(j, 1, 1).start()
        kept[j, 0] = got[:, sides[0]]
        got = multiply(j, bit0, bit1)
        for h in range(2):
            last[j, h] = got[:, sides[h]]

    for j in range(per):
        prepare(j)
    for j in range(per):
        scatter(j)
        fetch(j).wait()
        if j == 0:
            pl.semaphore_wait(barrier, 1 + depth * columns)
        products(j)
    for j in range(per):
        for h in range(2):
            stage_one(j, h, 0).wait_recv()
            second_out[j, h] = bf16(kept[j, h] + first_in[j, h, 0].astype(jnp.float32))
            stage_two(j, h).start()
    for j in range(per):
        for h in range(2):
            stage_one(j, h, 1).wait_recv()
            stage_two(j, h).wait_recv()
            total = (
                last[j, h]
                + first_in[j, h, 1].astype(jnp.float32)
                + second_in[j, h].astype(jnp.float32)
            )
            third_out[j, :, :, sides[h]] = bf16(total).reshape(depth * columns, share, half)
        others(lambda i, to_z, to_q: stage_three(j, i, to_z, to_q).start())
        third_in[j, z * columns + q] = third_out[j, z * columns + q]
    for j in range(per):
        others(lambda i, to_z, to_q: arrival(j, i).wait_recv())
        for c in range(columns):
            total = third_in[j, c].astype(jnp.float32)
            for k in range(1, depth):
                total = total + third_in[j, k * columns + c].astype(jnp.float32)
            out_ref[c * per + j] = total
    for j in range(per):
        for h in range(2):
            for part in range(2):
                stage_one(j, h, part).wait_send()
            stage_two(j, h).wait_send()
        others(lambda i, to_z, to_q: stage_three(j, i, to_z, to_q).wait_send())


def summed_signals(per, src, bins, fracs, gains):
    observers = gains.shape[1]
    rows = src.shape[0]
    shards, columns = lax.axis_size("gx"), lax.axis_size("gy")
    share = observers // (shards * columns)
    peers = shards // 4 * columns
    tall = peers * share
    half = NBIN // 2
    dma = pltpu.SemaphoreType.DMA
    return pl.pallas_call(
        functools.partial(spread_kernel, per, share),
        out_shape=jax.ShapeDtypeStruct((per * columns, share, NBIN), jnp.float32),
        in_specs=[pl.BlockSpec(memory_space=pltpu.VMEM)] * 3 + [pl.BlockSpec(memory_space=pl.ANY)],
        out_specs=pl.BlockSpec(memory_space=pltpu.VMEM),
        scratch_shapes=[
            pltpu.VMEM((per, observers, rows), jnp.bfloat16),
            pltpu.VMEM((per, 4, bins.shape[0], LANES), jnp.float32),
            pltpu.VMEM((rows, NBIN), jnp.bfloat16),
            pltpu.VMEM((per, 2, 2, tall, half), jnp.bfloat16),
            pltpu.VMEM((per, 2, 2, tall, half), jnp.bfloat16),
            pltpu.VMEM((per, 2, tall, half), jnp.float32),
            pltpu.VMEM((per, 2, tall, half), jnp.float32),
            pltpu.VMEM((per, 2, tall, half), jnp.bfloat16),
            pltpu.VMEM((per, 2, tall, half), jnp.bfloat16),
            pltpu.VMEM((per, peers, share, NBIN), jnp.bfloat16),
            pltpu.VMEM((per, peers, share, NBIN), jnp.bfloat16),
            dma((per,)),
            dma((per, 2, 2)),
            dma((per, 2, 2)),
            dma((per, 2)),
            dma((per, 2)),
            dma((per, peers)),
            dma((per, peers)),
        ],
        compiler_params=pltpu.CompilerParams(collective_id=0, has_side_effects=True),
        name="summed_signals",
    )(src, bins, fracs, gains)


def on_device(sources, owners, strip_rows, panel_counts, arrival_bins, arrival_fracs, gain_table):
    strip_count, terms, panels = sources.shape
    shards = lax.axis_size("gx")
    columns = lax.axis_size("gy")
    capacity = 2 * strip_count // shards
    blocks = arrival_bins.shape[1]
    observers = gain_table.shape[3]
    rows_here = arrival_bins.shape[0]
    live_mask = (jnp.arange(panels, dtype=jnp.int32)[None, :] < panel_counts[:, None]).astype(
        jnp.bfloat16
    )
    masked = (sources * live_mask[:, None, :]).reshape(strip_count, terms * panels)
    lane = jnp.arange(128, dtype=jnp.int32)[None, :]
    coded = jnp.where(
        lane == 0,
        (strip_rows // 128)[:, None],
        jnp.where(lane == 1, (strip_rows % 128)[:, None], jnp.where(lane == 2, 1, 0)),
    ).astype(jnp.bfloat16)
    payload = jnp.concatenate([masked, coded], axis=1)
    targets = owners[:, 0]
    earlier = (
        jnp.arange(strip_count, dtype=jnp.int32)[None, :]
        < jnp.arange(strip_count, dtype=jnp.int32)[:, None]
    )
    order_in = jnp.sum(
        jnp.where(earlier & (targets[None, :] == targets[:, None]), 1, 0).astype(jnp.int32), axis=1
    )
    slot_of = targets * capacity + order_in
    placing = jnp.arange(shards * capacity, dtype=jnp.int32)[:, None] == slot_of[None, :]
    send = jnp.dot(
        placing.astype(jnp.bfloat16), payload, preferred_element_type=jnp.float32
    ).astype(jnp.bfloat16)
    got = lax.all_to_all(send, "gx", split_axis=0, concat_axis=0, tiled=True)
    got = lax.all_gather(got, "gy", axis=0, tiled=True)
    codes = got[:, terms * panels :].astype(jnp.int32)
    got_rows = jnp.where(codes[:, 2] > 0, codes[:, 0] * 128 + codes[:, 1], -1)
    row_hot = (jnp.arange(rows_here, dtype=jnp.int32)[:, None] == got_rows[None, :]).astype(
        jnp.bfloat16
    )
    row_sources = jnp.dot(
        row_hot, got[:, : terms * panels], preferred_element_type=jnp.float32
    ).astype(jnp.bfloat16)
    src = row_sources.reshape(rows_here * terms, panels)
    per = blocks // columns
    gains = turned_gains(per, gain_table)
    return summed_signals(per, src, arrival_bins, arrival_fracs, gains).transpose(1, 0, 2)


def solution(mesh):
    placed = (
        P(("gx", "gy"), None, None),
        P(("gx", "gy"), None),
        P(("gx", "gy")),
        P(("gx", "gy")),
        P("gx", None, None),
        P("gx", None, None),
        P("gx", None, None, None),
    )
    return jax.shard_map(
        on_device,
        mesh=mesh,
        in_specs=placed,
        out_specs=P(("gx", "gy"), None, None),
        check_vma=False,
    )
```

```python
import functools

import jax
import jax.numpy as jnp
from jax import lax
from jax.experimental import pallas as pl
from jax.experimental.pallas import tpu as pltpu
from jax.sharding import PartitionSpec as P

NBIN = 256
LANES = 128
LO = 64
HI = NBIN // LO
WIDE = LO + 16
CHUNK = 128
SLOTS = 4
UNROLL = 16
MESH = pl.DeviceIdType.MESH


def bf16(v):
    return v.astype(jnp.bfloat16)


def aligned(i, n):
    return pl.multiple_of(i * n, n)


def signals_kernel(
    per, share, cap, sources_ref, owners_ref, owners_row_ref, strip_rows_ref, counts_ref, bins_ref, fracs_ref,
    gains_hbm, out_ref,
    gains, buffer, mixed, work, posted, got_in, row_sums,
    table, arrived, first_out, first_in, kept, last, second_out, second_in, third_out, third_in,
    gain_sems, post_send, post_recv, pass_send, pass_recv,
    one_send, one_recv, two_send, two_recv, three_send, three_recv,
):
    g = lax.axis_index("gx")
    q = lax.axis_index("gy")
    shards = lax.axis_size("gx")
    columns = lax.axis_size("gy")
    depth = shards // 4
    bit0, bit1, z = lax.rem(g, 2), lax.rem(g // 2, 2), g // 4
    flips = (g + 1 - 2 * bit0, g + 2 - 4 * bit1)
    corner = lax.rem(g, 4)
    rows = bins_ref.shape[0]
    wide = columns * share
    tall = depth * wide
    half = NBIN // 2

    observers = gains.shape[1]
    tiles_wide = observers // LANES
    blocks = bins_ref.shape[1]
    deep = tiles_wide * blocks
    group = 256 // deep
    steps = gains.shape[2] // CHUNK
    size = CHUNK * deep

    def fetch(i):
        slot = lax.rem(i, SLOTS)
        return pltpu.make_async_copy(
            gains_hbm.at[pl.ds(aligned(i, size), size)], buffer.at[slot], gain_sems.at[slot]
        )

    for i in range(SLOTS - 1):
        fetch(i).start()

    barrier = pltpu.get_barrier_semaphore()

    def greet(to_g, to_q):
        pl.semaphore_signal(barrier, inc=1, device_id=(to_g, to_q), device_id_type=MESH)

    def others(body):
        def one(i, c):
            to_z, to_q = i // columns, lax.rem(i, columns)

            @pl.when(jnp.logical_or(to_z != z, to_q != q))
            def _():
                body(i, to_z, to_q)

            return c

        lax.fori_loop(0, depth * columns, one, 0)

    def ring(body):
        def one(i, c):
            body(lax.rem(g + i, shards))
            return c

        lax.fori_loop(1, shards, one, 0)

    ring(lambda to_g: greet(to_g, q))

    def beside(body):
        def one(i, c):
            body(lax.rem(q + i, columns))
            return c

        lax.fori_loop(1, columns, one, 0)

    def greet_column(to_q):
        def one(k, c):
            greet(k * 4 + corner, to_q)
            return c

        lax.fori_loop(0, depth, one, 0)

    beside(greet_column)

    strips, terms, panels = sources_ref.shape
    long = terms * panels
    work[...] = sources_ref[...].reshape(strips * terms, panels).astype(jnp.float32)
    before = lax.broadcasted_iota(jnp.int32, (strips, strips), 1) < lax.broadcasted_iota(
        jnp.int32, (strips, strips), 0
    )
    same = jnp.logical_and(owners_ref[...] == owners_row_ref[...], before)
    order = jnp.sum(same.astype(jnp.float32), axis=1, keepdims=True).astype(jnp.int32)
    spot_of = owners_ref[...] * cap + order
    placing = bf16(
        (spot_of == lax.broadcasted_iota(jnp.int32, (strips, shards * cap), 1)).astype(jnp.float32)
    )
    live = lax.broadcasted_iota(jnp.int32, (strips, panels), 1) < counts_ref[...]
    pieces = [
        bf16(jnp.where(live, work[pl.ds(k, strips, stride=terms), :], 0.0)) for k in range(terms)
    ]
    labels = (strip_rows_ref[...] + 1).astype(jnp.float32)
    pieces.append(
        bf16(jnp.where(lax.broadcasted_iota(jnp.int32, (strips, LANES), 1) == 0, labels, 0.0))
    )
    placed = bf16(
        lax.dot_general(
            placing,
            jnp.concatenate(pieces, axis=1),
            (((0,), (0,)), ((), ())),
            preferred_element_type=jnp.float32,
        )
    )
    posted[...] = placed.reshape(shards, cap, long + LANES)

    def post(to_g):
        return pltpu.make_async_remote_copy(
            src_ref=posted.at[to_g],
            dst_ref=got_in.at[q, g],
            send_sem=post_send.at[to_g],
            recv_sem=post_recv.at[g],
            device_id=(to_g, q),
            device_id_type=MESH,
        )

    def posted_by(from_g):
        return pltpu.make_async_remote_copy(
            src_ref=posted.at[from_g],
            dst_ref=got_in.at[q, from_g],
            send_sem=post_send.at[from_g],
            recv_sem=post_recv.at[from_g],
            device_id=(from_g, q),
            device_id_type=MESH,
        )

    def hand(from_g, to_q):
        return pltpu.make_async_remote_copy(
            src_ref=got_in.at[q, from_g],
            dst_ref=got_in.at[q, from_g],
            send_sem=pass_send.at[to_q, from_g],
            recv_sem=pass_recv.at[q, from_g],
            device_id=(g, to_q),
            device_id_type=MESH,
        )

    def handed_by(from_g, from_q):
        return pltpu.make_async_remote_copy(
            src_ref=got_in.at[from_q, from_g],
            dst_ref=got_in.at[from_q, from_g],
            send_sem=pass_send.at[from_q, from_g],
            recv_sem=pass_recv.at[from_q, from_g],
            device_id=(g, from_q),
            device_id_type=MESH,
        )

    pl.semaphore_wait(barrier, shards - 1 + depth * (columns - 1))
    ring(lambda to_g: post(to_g).start())
    got_in[q, g] = posted[g]
    beside(lambda to_q: hand(g, to_q).start())

    height = per * tiles_wide * group
    row = lax.broadcasted_iota(jnp.int32, (height, 256), 0)
    spot = lax.broadcasted_iota(jnp.int32, (height, 256), 1)
    wanted = (
        lax.rem(row, group) * deep
        + lax.rem(row // group, tiles_wide) * blocks
        + q * per
        + row // (group * tiles_wide)
    )
    pick = bf16((wanted == spot).astype(jnp.float32))

    def turn(i, carry):
        slot = lax.rem(i, SLOTS)

        @pl.when(i + SLOTS - 1 < steps)
        def _():
            fetch(i + SLOTS - 1).start()

        fetch(i).wait()

        def part(j, c):
            one = buffer[slot, pl.ds(aligned(j, 512), 256), :]
            two = buffer[slot, pl.ds(aligned(j, 512) + 256, 256), :]
            got = jnp.dot(
                pick, jnp.concatenate([one, two], axis=1), preferred_element_type=jnp.float32
            )
            for o in range(per):
                for t in range(tiles_wide):
                    at = (o * tiles_wide + t) * group
                    both = jnp.concatenate(
                        [got[at : at + group, :LANES], got[at : at + group, LANES:]], axis=0
                    )
                    mixed[
                        o, pl.ds(aligned(j, 2 * group), 2 * group), t * LANES : (t + 1) * LANES
                    ] = bf16(both)
            return c

        lax.fori_loop(0, CHUNK // (2 * group), part, 0, unroll=True)
        for o in range(per):
            for t in range(tiles_wide):
                gains[o, t * LANES : (t + 1) * LANES, pl.ds(aligned(i, CHUNK), CHUNK)] = mixed[
                    o, :, t * LANES : (t + 1) * LANES
                ].T
        return carry

    lax.fori_loop(0, steps, turn, 0)

    spots = bf16(lax.broadcasted_iota(jnp.int32, (WIDE, LANES), 0).astype(jnp.float32))
    lane = lax.broadcasted_iota(jnp.int32, (16, LANES), 1)
    upper = lax.broadcasted_iota(jnp.int32, (16, LANES), 0) < 8
    zero = jnp.zeros((), jnp.bfloat16)

    def prepare(j):
        block = q * per + j
        bins = bins_ref[:, pl.ds(block, 1), :].reshape(rows, LANES)
        fracs = fracs_ref[:, pl.ds(block, 1), :].reshape(rows, LANES)
        table[j, 0] = (bins // LO).astype(jnp.float32)
        table[j, 1] = lax.rem(bins, LO).astype(jnp.float32)
        table[j, 2] = 1.0 - fracs
        table[j, 3] = fracs

    def scatter(j):
        def spread(kind, row, n):
            return jnp.broadcast_to(table[j, kind, pl.ds(row, 1), :], (n, LANES))

        def weights_of(row):
            low = spread(1, row, WIDE)
            return jnp.where(
                spots == bf16(low),
                bf16(spread(2, row, WIDE)),
                jnp.where(spots == bf16(low + 1.0), bf16(spread(3, row, WIDE)), zero),
            )

        def pair(i, carry):
            both = bf16(row_sums[pl.ds(aligned(i, 16), 16), :])
            left = bf16(jnp.where(upper, spread(0, 2 * i, 16), -1.0))
            right = bf16(jnp.where(upper, -1.0, spread(0, 2 * i + 1, 16)))
            lhs = []
            for h in range(HI):
                at = jnp.asarray(h, jnp.bfloat16)
                lhs.append(
                    jnp.concatenate(
                        [jnp.where(left == at, both, zero), jnp.where(right == at, both, zero)], axis=1
                    )
                )
            rhs = jnp.concatenate([weights_of(2 * i), weights_of(2 * i + 1)], axis=1)
            got = lax.dot_general(
                jnp.concatenate(lhs, axis=0), rhs, (((1,), (1,)), ((), ())), preferred_element_type=jnp.float32
            )
            got = jnp.concatenate([got, jnp.zeros((16 * HI, LANES - WIDE), jnp.float32)], axis=1)
            tiles = []
            carried = None
            for t in range(NBIN // LANES):
                even = got[32 * t : 32 * t + 16, :]
                odd = pltpu.roll(got[32 * t + 16 : 32 * t + 32, :], LO, 1)
                tile = even + jnp.where(lane >= LO, odd, 0.0)
                if carried is not None:
                    tile = tile + jnp.where(lane < LO, carried, 0.0)
                carried = odd
                tiles.append(tile)
            arrived[pl.ds(aligned(i, 16), 16), :] = bf16(jnp.concatenate(tiles, axis=1))
            return carry

        lax.fori_loop(0, rows // 2, pair, 0, unroll=UNROLL)

    def multiply(j, c0, c1):
        lhs = jnp.concatenate(
            [
                gains[j, pl.ds(pl.multiple_of((k * 4 + c1 * 2 + c0) * wide, 8), wide), :]
                for k in range(depth)
            ],
            axis=0,
        )
        return jnp.dot(lhs, arrived[...], preferred_element_type=jnp.float32)

    def stage_one(j, h, part):
        return pltpu.make_async_remote_copy(
            src_ref=first_out.at[j, h, part],
            dst_ref=first_in.at[j, h, part],
            send_sem=one_send.at[j, h, part],
            recv_sem=one_recv.at[j, h, part],
            device_id=(flips[h], q),
            device_id_type=MESH,
        )

    def stage_two(j, h):
        return pltpu.make_async_remote_copy(
            src_ref=second_out.at[j, h],
            dst_ref=second_in.at[j, h],
            send_sem=two_send.at[j, h],
            recv_sem=two_recv.at[j, h],
            device_id=(flips[1 - h], q),
            device_id_type=MESH,
        )

    def stage_three(j, i, to_z, to_q):
        return pltpu.make_async_remote_copy(
            src_ref=third_out.at[j, i],
            dst_ref=third_in.at[j, z * columns + q],
            send_sem=three_send.at[j, i],
            recv_sem=three_recv.at[j, z * columns + q],
            device_id=(to_z * 4 + corner, to_q),
            device_id_type=MESH,
        )

    def arrival(j, i):
        return pltpu.make_async_remote_copy(
            src_ref=third_out.at[j, i],
            dst_ref=third_in.at[j, i],
            send_sem=three_send.at[j, i],
            recv_sem=three_recv.at[j, i],
            device_id=((i // columns) * 4 + corner, lax.rem(i, columns)),
            device_id_type=MESH,
        )

    sides = (slice(0, half), slice(half, NBIN))

    def products(j):
        got = multiply(j, 1 - bit0, 1 - bit1)
        for h in range(2):
            first_out[j, h, 0] = bf16(got[:, sides[h]])
            stage_one(j, h, 0).start()
        got = multiply(j, 1 - bit0, bit1)
        first_out[j, 0, 1] = bf16(got[:, sides[0]])
        stage_one(j, 0, 1).start()
        kept[j, 1] = got[:, sides[1]]
        got = multiply(j, bit0, 1 - bit1)
        first_out[j, 1, 1] = bf16(got[:, sides[1]])
        stage_one(j, 1, 1).start()
        kept[j, 0] = got[:, sides[0]]
        got = multiply(j, bit0, bit1)
        for h in range(2):
            last[j, h] = got[:, sides[h]]

    for j in range(per):
        prepare(j)

    def relay(from_g):
        posted_by(from_g).wait_recv()
        beside(lambda to_q: hand(from_g, to_q).start())

    ring(relay)

    def every(body):
        def one(i, c):
            body(i)
            return c

        lax.fori_loop(0, shards, one, 0)

    beside(lambda from_q: every(lambda from_g: handed_by(from_g, from_q).wait_recv()))
    slots = columns * shards * cap
    letters = got_in[...].reshape(slots, long + LANES)
    labels = letters[:, long:].astype(jnp.float32)[:, :1] - 1.0
    hot = bf16(
        (labels == lax.broadcasted_iota(jnp.int32, (slots, rows), 1).astype(jnp.float32)).astype(jnp.float32)
    )
    summed = lax.dot_general(
        hot, letters[:, :long], (((0,), (0,)), ((), ())), preferred_element_type=jnp.float32
    )
    for k in range(terms):
        row_sums[pl.ds(k, rows, stride=terms), :] = summed[:, k * panels : (k + 1) * panels]
    for j in range(per):
        scatter(j)
        products(j)
    for j in range(per):
        for h in range(2):
            stage_one(j, h, 0).wait_recv()
            second_out[j, h] = bf16(kept[j, h] + first_in[j, h, 0].astype(jnp.float32))
            stage_two(j, h).start()
    for j in range(per):
        for h in range(2):
            stage_one(j, h, 1).wait_recv()
            stage_two(j, h).wait_recv()
            total = (
                last[j, h]
                + first_in[j, h, 1].astype(jnp.float32)
                + second_in[j, h].astype(jnp.float32)
            )
            third_out[j, :, :, sides[h]] = bf16(total).reshape(depth * columns, share, half)
        others(lambda i, to_z, to_q: stage_three(j, i, to_z, to_q).start())
        third_in[j, z * columns + q] = third_out[j, z * columns + q]
    for j in range(per):
        others(lambda i, to_z, to_q: arrival(j, i).wait_recv())
        for c in range(columns):
            total = third_in[j, c].astype(jnp.float32)
            for k in range(1, depth):
                total = total + third_in[j, k * columns + c].astype(jnp.float32)
            out_ref[c * per + j] = total
    for j in range(per):
        for h in range(2):
            for part in range(2):
                stage_one(j, h, part).wait_send()
            stage_two(j, h).wait_send()
        others(lambda i, to_z, to_q: stage_three(j, i, to_z, to_q).wait_send())
    ring(lambda to_g: post(to_g).wait_send())
    beside(lambda to_q: every(lambda from_g: hand(from_g, to_q).wait_send()))


def on_device(sources, owners, strip_rows, panel_counts, arrival_bins, arrival_fracs, gain_table):
    strips, terms, panels = sources.shape
    shards, columns = lax.axis_size("gx"), lax.axis_size("gy")
    cap = 2 * strips // shards
    rows, blocks = arrival_bins.shape[:2]
    observers = gain_table.shape[3]
    per = blocks // columns
    share = observers // (shards * columns)
    peers = shards // 4 * columns
    tall = peers * share
    half = NBIN // 2
    tiles_wide = observers // LANES
    wide = terms * panels + LANES
    assert panels == LANES and rows <= 256 and terms == 8
    flat = (
        gain_table.reshape(rows * terms, blocks, tiles_wide, LANES).transpose(0, 2, 1, 3).reshape(-1, LANES)
    )
    dma = pltpu.SemaphoreType.DMA
    signals = pl.pallas_call(
        functools.partial(signals_kernel, per, share, cap),
        out_shape=jax.ShapeDtypeStruct((blocks, share, NBIN), jnp.float32),
        in_specs=[pl.BlockSpec(memory_space=pltpu.VMEM)] * 7 + [pl.BlockSpec(memory_space=pl.ANY)],
        out_specs=pl.BlockSpec(memory_space=pltpu.VMEM),
        scratch_shapes=[
            pltpu.VMEM((per, observers, rows * terms), jnp.bfloat16),
            pltpu.VMEM((SLOTS, CHUNK * tiles_wide * blocks, LANES), jnp.bfloat16),
            pltpu.VMEM((per, CHUNK, observers), jnp.bfloat16),
            pltpu.VMEM((strips * terms, panels), jnp.float32),
            pltpu.VMEM((shards, cap, wide), jnp.bfloat16),
            pltpu.VMEM((columns, shards, cap, wide), jnp.bfloat16),
            pltpu.VMEM((rows * terms, panels), jnp.float32),
            pltpu.VMEM((per, 4, rows, LANES), jnp.float32),
            pltpu.VMEM((rows * terms, NBIN), jnp.bfloat16),
            pltpu.VMEM((per, 2, 2, tall, half), jnp.bfloat16),
            pltpu.VMEM((per, 2, 2, tall, half), jnp.bfloat16),
            pltpu.VMEM((per, 2, tall, half), jnp.float32),
            pltpu.VMEM((per, 2, tall, half), jnp.float32),
            pltpu.VMEM((per, 2, tall, half), jnp.bfloat16),
            pltpu.VMEM((per, 2, tall, half), jnp.bfloat16),
            pltpu.VMEM((per, peers, share, NBIN), jnp.bfloat16),
            pltpu.VMEM((per, peers, share, NBIN), jnp.bfloat16),
            dma((SLOTS,)),
            dma((shards,)),
            dma((shards,)),
            dma((columns, shards)),
            dma((columns, shards)),
            dma((per, 2, 2)),
            dma((per, 2, 2)),
            dma((per, 2)),
            dma((per, 2)),
            dma((per, peers)),
            dma((per, peers)),
        ],
        compiler_params=pltpu.CompilerParams(collective_id=0, has_side_effects=True),
        name="signals",
    )(
        sources,
        owners,
        owners.reshape(1, strips),
        strip_rows.reshape(strips, 1),
        panel_counts.reshape(strips, 1),
        arrival_bins,
        arrival_fracs,
        flat,
    )
    return signals.transpose(1, 0, 2)


def solution(mesh):
    placed = (
        P(("gx", "gy"), None, None),
        P(("gx", "gy"), None),
        P(("gx", "gy")),
        P(("gx", "gy")),
        P("gx", None, None),
        P("gx", None, None),
        P("gx", None, None, None),
    )
    return jax.shard_map(
        on_device,
        mesh=mesh,
        in_specs=placed,
        out_specs=P(("gx", "gy"), None, None),
        check_vma=False,
    )
```

```python
import functools

import jax
import jax.numpy as jnp
from jax import lax
from jax.experimental import pallas as pl
from jax.experimental.pallas import tpu as pltpu
from jax.sharding import PartitionSpec as P

NBIN = 256
LANES = 128
LO = 64
HI = NBIN // LO
WIDE = LO + 16
CHUNK = 128
SLOTS = 4
UNROLL = 16
MESH = pl.DeviceIdType.MESH


def bf16(v):
    return v.astype(jnp.bfloat16)


def aligned(i, n):
    return pl.multiple_of(i * n, n)


def signals_kernel(
    per, share, cap, sources_ref, owners_ref, strip_rows_ref, counts_ref, bins_ref, fracs_ref,
    gains_hbm, out_ref,
    gains, buffer, mixed, work, posted, got_in, row_sums,
    table, arrived, first_out, first_in, kept, last, second_out, second_in, third_out, third_in,
    gain_sems, post_send, post_recv, pass_send, pass_recv,
    one_send, one_recv, two_send, two_recv, three_send, three_recv,
):
    g = lax.axis_index("gx")
    q = lax.axis_index("gy")
    shards = lax.axis_size("gx")
    columns = lax.axis_size("gy")
    depth = shards // 4
    bit0, bit1, z = lax.rem(g, 2), lax.rem(g // 2, 2), g // 4
    flips = (g + 1 - 2 * bit0, g + 2 - 4 * bit1)
    corner = lax.rem(g, 4)
    rows = bins_ref.shape[0]
    wide = columns * share
    tall = depth * wide
    half = NBIN // 2

    observers = gains.shape[1]
    tiles_wide = observers // LANES
    blocks = bins_ref.shape[1]
    deep = tiles_wide * blocks
    group = 256 // deep
    steps = gains.shape[2] // CHUNK
    size = CHUNK * deep

    def fetch(i):
        slot = lax.rem(i, SLOTS)
        return pltpu.make_async_copy(
            gains_hbm.at[pl.ds(aligned(i, size), size)], buffer.at[slot], gain_sems.at[slot]
        )

    for i in range(SLOTS - 1):
        fetch(i).start()

    barrier = pltpu.get_barrier_semaphore()

    def greet(to_g, to_q):
        pl.semaphore_signal(barrier, inc=1, device_id=(to_g, to_q), device_id_type=MESH)

    def others(body):
        def one(i, c):
            to_z, to_q = i // columns, lax.rem(i, columns)

            @pl.when(jnp.logical_or(to_z != z, to_q != q))
            def _():
                body(i, to_z, to_q)

            return c

        lax.fori_loop(0, depth * columns, one, 0)

    def ring(body):
        def one(i, c):
            body(lax.rem(g + i, shards))
            return c

        lax.fori_loop(1, shards, one, 0)

    ring(lambda to_g: greet(to_g, q))

    def beside(body):
        def one(i, c):
            body(lax.rem(q + i, columns))
            return c

        lax.fori_loop(1, columns, one, 0)

    def greet_column(to_q):
        def one(k, c):
            greet(k * 4 + corner, to_q)
            return c

        lax.fori_loop(0, depth, one, 0)

    beside(greet_column)

    strips, terms, panels = sources_ref.shape
    long = terms * panels
    work[...] = sources_ref[...].reshape(strips * terms, panels).astype(jnp.float32)
    before = lax.broadcasted_iota(jnp.int32, (strips, strips), 1) < lax.broadcasted_iota(
        jnp.int32, (strips, strips), 0
    )
    eye = lax.broadcasted_iota(jnp.int32, (strips, strips), 1) == lax.broadcasted_iota(
        jnp.int32, (strips, strips), 0
    )

    def stood(ref):
        row = ref[...].astype(jnp.float32)
        return jnp.sum(jnp.where(eye, jnp.broadcast_to(row, eye.shape), 0.0), axis=1, keepdims=True)

    targets = stood(owners_ref)
    same = jnp.logical_and(targets == owners_ref[...].astype(jnp.float32), before)
    order = jnp.sum(same.astype(jnp.float32), axis=1, keepdims=True)
    spot_of = (targets * cap + order).astype(jnp.int32)
    placing = bf16(
        (spot_of == lax.broadcasted_iota(jnp.int32, (strips, shards * cap), 1)).astype(jnp.float32)
    )
    live = lax.broadcasted_iota(jnp.int32, (strips, panels), 1).astype(jnp.float32) < stood(counts_ref)
    pieces = [
        bf16(jnp.where(live, work[pl.ds(k, strips, stride=terms), :], 0.0)) for k in range(terms)
    ]
    labels = stood(strip_rows_ref) + 1.0
    pieces.append(
        bf16(jnp.where(lax.broadcasted_iota(jnp.int32, (strips, LANES), 1) == 0, labels, 0.0))
    )
    placed = bf16(
        lax.dot_general(
            placing,
            jnp.concatenate(pieces, axis=1),
            (((0,), (0,)), ((), ())),
            preferred_element_type=jnp.float32,
        )
    )
    posted[...] = placed.reshape(shards, cap, long + LANES)

    def post(to_g):
        return pltpu.make_async_remote_copy(
            src_ref=posted.at[to_g],
            dst_ref=got_in.at[q, g],
            send_sem=post_send.at[to_g],
            recv_sem=post_recv.at[g],
            device_id=(to_g, q),
            device_id_type=MESH,
        )

    def posted_by(from_g):
        return pltpu.make_async_remote_copy(
            src_ref=posted.at[from_g],
            dst_ref=got_in.at[q, from_g],
            send_sem=post_send.at[from_g],
            recv_sem=post_recv.at[from_g],
            device_id=(from_g, q),
            device_id_type=MESH,
        )

    def hand(from_g, to_q):
        return pltpu.make_async_remote_copy(
            src_ref=got_in.at[q, from_g],
            dst_ref=got_in.at[q, from_g],
            send_sem=pass_send.at[to_q, from_g],
            recv_sem=pass_recv.at[q, from_g],
            device_id=(g, to_q),
            device_id_type=MESH,
        )

    def handed_by(from_g, from_q):
        return pltpu.make_async_remote_copy(
            src_ref=got_in.at[from_q, from_g],
            dst_ref=got_in.at[from_q, from_g],
            send_sem=pass_send.at[from_q, from_g],
            recv_sem=pass_recv.at[from_q, from_g],
            device_id=(g, from_q),
            device_id_type=MESH,
        )

    pl.semaphore_wait(barrier, shards - 1 + depth * (columns - 1))
    ring(lambda to_g: post(to_g).start())
    got_in[q, g] = posted[g]
    beside(lambda to_q: hand(g, to_q).start())

    height = per * tiles_wide * group
    row = lax.broadcasted_iota(jnp.int32, (height, 256), 0)
    spot = lax.broadcasted_iota(jnp.int32, (height, 256), 1)
    wanted = (
        lax.rem(row, group) * deep
        + lax.rem(row // group, tiles_wide) * blocks
        + q * per
        + row // (group * tiles_wide)
    )
    pick = bf16((wanted == spot).astype(jnp.float32))

    def turn(i, carry):
        slot = lax.rem(i, SLOTS)

        @pl.when(i + SLOTS - 1 < steps)
        def _():
            fetch(i + SLOTS - 1).start()

        fetch(i).wait()

        def part(j, c):
            one = buffer[slot, pl.ds(aligned(j, 512), 256), :]
            two = buffer[slot, pl.ds(aligned(j, 512) + 256, 256), :]
            got = jnp.dot(
                pick, jnp.concatenate([one, two], axis=1), preferred_element_type=jnp.float32
            )
            for o in range(per):
                for t in range(tiles_wide):
                    at = (o * tiles_wide + t) * group
                    both = jnp.concatenate(
                        [got[at : at + group, :LANES], got[at : at + group, LANES:]], axis=0
                    )
                    mixed[
                        o, pl.ds(aligned(j, 2 * group), 2 * group), t * LANES : (t + 1) * LANES
                    ] = bf16(both)
            return c

        lax.fori_loop(0, CHUNK // (2 * group), part, 0, unroll=True)
        for o in range(per):
            for t in range(tiles_wide):
                gains[o, t * LANES : (t + 1) * LANES, pl.ds(aligned(i, CHUNK), CHUNK)] = mixed[
                    o, :, t * LANES : (t + 1) * LANES
                ].T
        return carry

    lax.fori_loop(0, steps, turn, 0)

    spots = bf16(lax.broadcasted_iota(jnp.int32, (WIDE, LANES), 0).astype(jnp.float32))
    lane = lax.broadcasted_iota(jnp.int32, (16, LANES), 1)
    upper = lax.broadcasted_iota(jnp.int32, (16, LANES), 0) < 8
    zero = jnp.zeros((), jnp.bfloat16)

    def prepare(j):
        block = q * per + j
        bins = bins_ref[:, pl.ds(block, 1), :].reshape(rows, LANES)
        fracs = fracs_ref[:, pl.ds(block, 1), :].reshape(rows, LANES)
        table[j, 0] = (bins // LO).astype(jnp.float32)
        table[j, 1] = lax.rem(bins, LO).astype(jnp.float32)
        table[j, 2] = 1.0 - fracs
        table[j, 3] = fracs

    def scatter(j, low, high):
        def spread(kind, row, n):
            return jnp.broadcast_to(table[j, kind, pl.ds(row, 1), :], (n, LANES))

        def weights_of(row):
            low = spread(1, row, WIDE)
            return jnp.where(
                spots == bf16(low),
                bf16(spread(2, row, WIDE)),
                jnp.where(spots == bf16(low + 1.0), bf16(spread(3, row, WIDE)), zero),
            )

        def pair(i, carry):
            both = bf16(row_sums[pl.ds(aligned(i, 16), 16), :])
            left = bf16(jnp.where(upper, spread(0, 2 * i, 16), -1.0))
            right = bf16(jnp.where(upper, -1.0, spread(0, 2 * i + 1, 16)))
            lhs = []
            for h in range(HI):
                at = jnp.asarray(h, jnp.bfloat16)
                lhs.append(
                    jnp.concatenate(
                        [jnp.where(left == at, both, zero), jnp.where(right == at, both, zero)], axis=1
                    )
                )
            rhs = jnp.concatenate([weights_of(2 * i), weights_of(2 * i + 1)], axis=1)
            got = lax.dot_general(
                jnp.concatenate(lhs, axis=0), rhs, (((1,), (1,)), ((), ())), preferred_element_type=jnp.float32
            )
            got = jnp.concatenate([got, jnp.zeros((16 * HI, LANES - WIDE), jnp.float32)], axis=1)
            tiles = []
            carried = None
            for t in range(NBIN // LANES):
                even = got[32 * t : 32 * t + 16, :]
                odd = pltpu.roll(got[32 * t + 16 : 32 * t + 32, :], LO, 1)
                tile = even + jnp.where(lane >= LO, odd, 0.0)
                if carried is not None:
                    tile = tile + jnp.where(lane < LO, carried, 0.0)
                carried = odd
                tiles.append(tile)
            arrived[pl.ds(aligned(i, 16), 16), :] = bf16(jnp.concatenate(tiles, axis=1))
            return carry

        lax.fori_loop(low, high, pair, 0, unroll=UNROLL)

    def multiply(j, c0, c1):
        lhs = jnp.concatenate(
            [
                gains[j, pl.ds(pl.multiple_of((k * 4 + c1 * 2 + c0) * wide, 8), wide), :]
                for k in range(depth)
            ],
            axis=0,
        )
        return jnp.dot(lhs, arrived[...], preferred_element_type=jnp.float32)

    def stage_one(j, h, part):
        return pltpu.make_async_remote_copy(
            src_ref=first_out.at[j, h, part],
            dst_ref=first_in.at[j, h, part],
            send_sem=one_send.at[j, h, part],
            recv_sem=one_recv.at[j, h, part],
            device_id=(flips[h], q),
            device_id_type=MESH,
        )

    def stage_two(j, h):
        return pltpu.make_async_remote_copy(
            src_ref=second_out.at[j, h],
            dst_ref=second_in.at[j, h],
            send_sem=two_send.at[j, h],
            recv_sem=two_recv.at[j, h],
            device_id=(flips[1 - h], q),
            device_id_type=MESH,
        )

    def stage_three(j, i, to_z, to_q):
        return pltpu.make_async_remote_copy(
            src_ref=third_out.at[j, i],
            dst_ref=third_in.at[j, z * columns + q],
            send_sem=three_send.at[j, i],
            recv_sem=three_recv.at[j, z * columns + q],
            device_id=(to_z * 4 + corner, to_q),
            device_id_type=MESH,
        )

    def arrival(j, i):
        return pltpu.make_async_remote_copy(
            src_ref=third_out.at[j, i],
            dst_ref=third_in.at[j, i],
            send_sem=three_send.at[j, i],
            recv_sem=three_recv.at[j, i],
            device_id=((i // columns) * 4 + corner, lax.rem(i, columns)),
            device_id_type=MESH,
        )

    sides = (slice(0, half), slice(half, NBIN))

    def products(j):
        got = multiply(j, 1 - bit0, 1 - bit1)
        for h in range(2):
            first_out[j, h, 0] = bf16(got[:, sides[h]])
            stage_one(j, h, 0).start()
        got = multiply(j, 1 - bit0, bit1)
        first_out[j, 0, 1] = bf16(got[:, sides[0]])
        stage_one(j, 0, 1).start()
        kept[j, 1] = got[:, sides[1]]
        got = multiply(j, bit0, 1 - bit1)
        first_out[j, 1, 1] = bf16(got[:, sides[1]])
        stage_one(j, 1, 1).start()
        kept[j, 0] = got[:, sides[0]]
        got = multiply(j, bit0, bit1)
        for h in range(2):
            last[j, h] = got[:, sides[h]]

    for j in range(per):
        prepare(j)

    def relay(from_g):
        posted_by(from_g).wait_recv()
        beside(lambda to_q: hand(from_g, to_q).start())

    ring(relay)

    def every(body):
        def one(i, c):
            body(i)
            return c

        lax.fori_loop(0, shards, one, 0)

    beside(lambda from_q: every(lambda from_g: handed_by(from_g, from_q).wait_recv()))
    slots = columns * shards * cap
    letters = got_in[...].reshape(slots, long + LANES)
    labels = letters[:, long:].astype(jnp.float32)[:, :1] - 1.0
    hot = bf16(
        (labels == lax.broadcasted_iota(jnp.int32, (slots, rows), 1).astype(jnp.float32)).astype(jnp.float32)
    )
    summed = lax.dot_general(
        hot, letters[:, :long], (((0,), (0,)), ((), ())), preferred_element_type=jnp.float32
    )
    for k in range(terms):
        row_sums[pl.ds(k, rows, stride=terms), :] = summed[:, k * panels : (k + 1) * panels]
    def second(j):
        for h in range(2):
            stage_one(j, h, 0).wait_recv()
            second_out[j, h] = bf16(kept[j, h] + first_in[j, h, 0].astype(jnp.float32))
            stage_two(j, h).start()

    def third(j):
        for h in range(2):
            stage_one(j, h, 1).wait_recv()
            stage_two(j, h).wait_recv()
            total = (
                last[j, h]
                + first_in[j, h, 1].astype(jnp.float32)
                + second_in[j, h].astype(jnp.float32)
            )
            third_out[j, :, :, sides[h]] = bf16(total).reshape(depth * columns, share, half)
        others(lambda i, to_z, to_q: stage_three(j, i, to_z, to_q).start())
        third_in[j, z * columns + q] = third_out[j, z * columns + q]

    pairs = rows // 2
    for j in range(per):
        if j == 0:
            scatter(j, 0, pairs)
        else:
            scatter(j, 0, pairs // 2)
            second(j - 1)
            scatter(j, pairs // 2, pairs)
        products(j)
        if j > 0:
            third(j - 1)
    second(per - 1)
    third(per - 1)
    for j in range(per):
        others(lambda i, to_z, to_q: arrival(j, i).wait_recv())
        for c in range(columns):
            total = third_in[j, c].astype(jnp.float32)
            for k in range(1, depth):
                total = total + third_in[j, k * columns + c].astype(jnp.float32)
            out_ref[:, c * per + j, :] = total
    for j in range(per):
        for h in range(2):
            for part in range(2):
                stage_one(j, h, part).wait_send()
            stage_two(j, h).wait_send()
        others(lambda i, to_z, to_q: stage_three(j, i, to_z, to_q).wait_send())
    ring(lambda to_g: post(to_g).wait_send())
    beside(lambda to_q: every(lambda from_g: hand(from_g, to_q).wait_send()))


def on_device(sources, owners, strip_rows, panel_counts, arrival_bins, arrival_fracs, gain_table):
    strips, terms, panels = sources.shape
    shards, columns = lax.axis_size("gx"), lax.axis_size("gy")
    cap = 2 * strips // shards
    rows, blocks = arrival_bins.shape[:2]
    observers = gain_table.shape[3]
    per = blocks // columns
    share = observers // (shards * columns)
    peers = shards // 4 * columns
    tall = peers * share
    half = NBIN // 2
    tiles_wide = observers // LANES
    wide = terms * panels + LANES
    assert panels == LANES and rows <= 256 and terms == 8
    flat = (
        gain_table.reshape(rows * terms, blocks, tiles_wide, LANES).transpose(0, 2, 1, 3).reshape(-1, LANES)
    )
    dma = pltpu.SemaphoreType.DMA
    return pl.pallas_call(
        functools.partial(signals_kernel, per, share, cap),
        out_shape=jax.ShapeDtypeStruct((share, blocks, NBIN), jnp.float32),
        in_specs=[pl.BlockSpec(memory_space=pltpu.VMEM)] * 6 + [pl.BlockSpec(memory_space=pl.ANY)],
        out_specs=pl.BlockSpec(memory_space=pltpu.VMEM),
        scratch_shapes=[
            pltpu.VMEM((per, observers, rows * terms), jnp.bfloat16),
            pltpu.VMEM((SLOTS, CHUNK * tiles_wide * blocks, LANES), jnp.bfloat16),
            pltpu.VMEM((per, CHUNK, observers), jnp.bfloat16),
            pltpu.VMEM((strips * terms, panels), jnp.float32),
            pltpu.VMEM((shards, cap, wide), jnp.bfloat16),
            pltpu.VMEM((columns, shards, cap, wide), jnp.bfloat16),
            pltpu.VMEM((rows * terms, panels), jnp.float32),
            pltpu.VMEM((per, 4, rows, LANES), jnp.float32),
            pltpu.VMEM((rows * terms, NBIN), jnp.bfloat16),
            pltpu.VMEM((per, 2, 2, tall, half), jnp.bfloat16),
            pltpu.VMEM((per, 2, 2, tall, half), jnp.bfloat16),
            pltpu.VMEM((per, 2, tall, half), jnp.float32),
            pltpu.VMEM((per, 2, tall, half), jnp.float32),
            pltpu.VMEM((per, 2, tall, half), jnp.bfloat16),
            pltpu.VMEM((per, 2, tall, half), jnp.bfloat16),
            pltpu.VMEM((per, peers, share, NBIN), jnp.bfloat16),
            pltpu.VMEM((per, peers, share, NBIN), jnp.bfloat16),
            dma((SLOTS,)),
            dma((shards,)),
            dma((shards,)),
            dma((columns, shards)),
            dma((columns, shards)),
            dma((per, 2, 2)),
            dma((per, 2, 2)),
            dma((per, 2)),
            dma((per, 2)),
            dma((per, peers)),
            dma((per, peers)),
        ],
        compiler_params=pltpu.CompilerParams(collective_id=0, has_side_effects=True),
        name="signals",
    )(
        sources,
        owners.reshape(1, strips),
        strip_rows.reshape(1, strips),
        panel_counts.reshape(1, strips),
        arrival_bins,
        arrival_fracs,
        flat,
    )


def solution(mesh):
    placed = (
        P(("gx", "gy"), None, None),
        P(("gx", "gy"), None),
        P(("gx", "gy")),
        P(("gx", "gy")),
        P("gx", None, None),
        P("gx", None, None),
        P("gx", None, None, None),
    )
    return jax.shard_map(
        on_device,
        mesh=mesh,
        in_specs=placed,
        out_specs=P(("gx", "gy"), None, None),
        check_vma=False,
    )
```

```python
import functools

import jax
import jax.numpy as jnp
from jax import lax
from jax.experimental import pallas as pl
from jax.experimental.pallas import tpu as pltpu
from jax.sharding import PartitionSpec as P

NBIN = 256
LANES = 128
LO = 64
LO_BITS = LO.bit_length() - 1
HI = NBIN // LO
WIDE = LO + 16
CHUNK = 128
SLOTS = 4
UNROLL = 64
MESH = pl.DeviceIdType.MESH


def bf16(v):
    return v.astype(jnp.bfloat16)


def aligned(i, n):
    return pl.multiple_of(i * n, n)


def signals_kernel(
    per, share, cap, sources_ref, owners_ref, strip_rows_ref, counts_ref,
    bins_hbm, fracs_hbm, gains_hbm, out_ref,
    gains, buffer, mixed, work, posted, got_in, row_sums,
    bins, fracs, arrived, first_out, first_in, kept, last, second_out, second_in, third_out, third_in,
    gain_sems, table_sems, post_send, post_recv, pass_send, pass_recv,
    one_send, one_recv, two_send, two_recv, three_send, three_recv,
):
    g = lax.axis_index("gx")
    q = lax.axis_index("gy")
    shards = lax.axis_size("gx")
    columns = lax.axis_size("gy")
    depth = shards // 4
    bit0, bit1, z = lax.rem(g, 2), lax.rem(g // 2, 2), g // 4
    flips = (g + 1 - 2 * bit0, g + 2 - 4 * bit1)
    corner = lax.rem(g, 4)
    rows = row_sums.shape[0] // 8
    wide = columns * share
    tall = depth * wide
    half = NBIN // 2

    observers = gains.shape[1]
    tiles_wide = observers // LANES
    blocks = per * columns
    deep = tiles_wide * blocks
    group = 256 // deep
    steps = gains.shape[2] // CHUNK
    size = CHUNK * deep

    def fetch(i):
        slot = lax.rem(i, SLOTS)
        return pltpu.make_async_copy(
            gains_hbm.at[pl.ds(aligned(i, size), size)], buffer.at[slot], gain_sems.at[slot]
        )

    for i in range(SLOTS - 1):
        fetch(i).start()
    tables = (
        pltpu.make_async_copy(bins_hbm, bins, table_sems.at[0]),
        pltpu.make_async_copy(fracs_hbm, fracs, table_sems.at[1]),
    )
    for table in tables:
        table.start()

    barrier = pltpu.get_barrier_semaphore()

    def greet(to_g, to_q):
        pl.semaphore_signal(barrier, inc=1, device_id=(to_g, to_q), device_id_type=MESH)

    def others(body):
        def one(i, c):
            to_z, to_q = i // columns, lax.rem(i, columns)

            @pl.when(jnp.logical_or(to_z != z, to_q != q))
            def _():
                body(i, to_z, to_q)

            return c

        lax.fori_loop(0, depth * columns, one, 0)

    def ring(body):
        def one(i, c):
            body(lax.rem(g + i, shards))
            return c

        lax.fori_loop(1, shards, one, 0)

    ring(lambda to_g: greet(to_g, q))

    def beside(body):
        def one(i, c):
            body(lax.rem(q + i, columns))
            return c

        lax.fori_loop(1, columns, one, 0)

    def greet_column(to_q):
        def one(k, c):
            greet(k * 4 + corner, to_q)
            return c

        lax.fori_loop(0, depth, one, 0)

    beside(greet_column)

    strips, terms, panels = sources_ref.shape
    long = terms * panels
    work[...] = sources_ref[...].reshape(strips * terms, panels).astype(jnp.float32)
    before = lax.broadcasted_iota(jnp.int32, (strips, strips), 1) < lax.broadcasted_iota(
        jnp.int32, (strips, strips), 0
    )
    eye = lax.broadcasted_iota(jnp.int32, (strips, strips), 1) == lax.broadcasted_iota(
        jnp.int32, (strips, strips), 0
    )

    def stood(ref):
        row = ref[...].astype(jnp.float32)
        return jnp.sum(jnp.where(eye, jnp.broadcast_to(row, eye.shape), 0.0), axis=1, keepdims=True)

    targets = stood(owners_ref)
    same = jnp.logical_and(targets == owners_ref[...].astype(jnp.float32), before)
    order = jnp.sum(same.astype(jnp.float32), axis=1, keepdims=True)
    spot_of = (targets * cap + order).astype(jnp.int32)
    placing = bf16(
        (spot_of == lax.broadcasted_iota(jnp.int32, (strips, shards * cap), 1)).astype(jnp.float32)
    )
    live = lax.broadcasted_iota(jnp.int32, (strips, panels), 1).astype(jnp.float32) < stood(counts_ref)
    pieces = [
        bf16(jnp.where(live, work[pl.ds(k, strips, stride=terms), :], 0.0)) for k in range(terms)
    ]
    labels = stood(strip_rows_ref) + 1.0
    pieces.append(
        bf16(jnp.where(lax.broadcasted_iota(jnp.int32, (strips, LANES), 1) == 0, labels, 0.0))
    )
    placed = bf16(
        lax.dot_general(
            placing,
            jnp.concatenate(pieces, axis=1),
            (((0,), (0,)), ((), ())),
            preferred_element_type=jnp.float32,
        )
    )
    posted[...] = placed.reshape(shards, cap, long + LANES)

    def post(to_g):
        return pltpu.make_async_remote_copy(
            src_ref=posted.at[to_g],
            dst_ref=got_in.at[q, g],
            send_sem=post_send.at[to_g],
            recv_sem=post_recv.at[g],
            device_id=(to_g, q),
            device_id_type=MESH,
        )

    def posted_by(from_g):
        return pltpu.make_async_remote_copy(
            src_ref=posted.at[from_g],
            dst_ref=got_in.at[q, from_g],
            send_sem=post_send.at[from_g],
            recv_sem=post_recv.at[from_g],
            device_id=(from_g, q),
            device_id_type=MESH,
        )

    def hand(from_g, to_q):
        return pltpu.make_async_remote_copy(
            src_ref=got_in.at[q, from_g],
            dst_ref=got_in.at[q, from_g],
            send_sem=pass_send.at[to_q, from_g],
            recv_sem=pass_recv.at[q, from_g],
            device_id=(g, to_q),
            device_id_type=MESH,
        )

    def handed_by(from_g, from_q):
        return pltpu.make_async_remote_copy(
            src_ref=got_in.at[from_q, from_g],
            dst_ref=got_in.at[from_q, from_g],
            send_sem=pass_send.at[from_q, from_g],
            recv_sem=pass_recv.at[from_q, from_g],
            device_id=(g, from_q),
            device_id_type=MESH,
        )

    pl.semaphore_wait(barrier, shards - 1 + depth * (columns - 1))
    turn_round = jnp.where(z * 2 < depth, shards - 1, 1)

    def far_first(i, c):
        post(lax.rem(g + i * turn_round, shards)).start()
        return c

    lax.fori_loop(1, shards, far_first, 0)
    got_in[q, g] = posted[g]
    beside(lambda to_q: hand(g, to_q).start())

    height = per * tiles_wide * group
    row = lax.broadcasted_iota(jnp.int32, (height, 256), 0)
    spot = lax.broadcasted_iota(jnp.int32, (height, 256), 1)
    wanted = (
        lax.rem(row, group) * deep
        + lax.rem(row // group, tiles_wide) * blocks
        + q * per
        + row // (group * tiles_wide)
    )
    pick = bf16((wanted == spot).astype(jnp.float32))

    def turn(i, carry):
        slot = lax.rem(i, SLOTS)

        @pl.when(i + SLOTS - 1 < steps)
        def _():
            fetch(i + SLOTS - 1).start()

        fetch(i).wait()

        def part(j, c):
            one = buffer[slot, pl.ds(aligned(j, 512), 256), :]
            two = buffer[slot, pl.ds(aligned(j, 512) + 256, 256), :]
            got = jnp.dot(
                pick, jnp.concatenate([one, two], axis=1), preferred_element_type=jnp.float32
            )
            for o in range(per):
                for t in range(tiles_wide):
                    at = (o * tiles_wide + t) * group
                    both = jnp.concatenate(
                        [got[at : at + group, :LANES], got[at : at + group, LANES:]], axis=0
                    )
                    mixed[
                        o, pl.ds(aligned(j, 2 * group), 2 * group), t * LANES : (t + 1) * LANES
                    ] = bf16(both)
            return c

        lax.fori_loop(0, CHUNK // (2 * group), part, 0, unroll=True)
        for o in range(per):
            for t in range(tiles_wide):
                gains[o, t * LANES : (t + 1) * LANES, pl.ds(aligned(i, CHUNK), CHUNK)] = mixed[
                    o, :, t * LANES : (t + 1) * LANES
                ].T
        return carry

    lax.fori_loop(0, steps, turn, 0)
    for table in tables:
        table.wait()

    spots = bf16(lax.broadcasted_iota(jnp.int32, (WIDE, LANES), 0).astype(jnp.float32))
    lane = lax.broadcasted_iota(jnp.int32, (16, LANES), 1)
    upper = lax.broadcasted_iota(jnp.int32, (16, LANES), 0) < 8
    zero = jnp.zeros((), jnp.bfloat16)

    def scatter(j, low, high):
        block = q * per + j

        def spread(ref, row, n):
            return jnp.broadcast_to(ref[pl.ds(row * blocks + block, 1), :], (n, LANES))

        def weights_of(row):
            frac = spread(fracs, row, WIDE)
            low = (spread(bins, row, WIDE) & (LO - 1)).astype(jnp.float32)
            return jnp.where(
                spots == bf16(low),
                bf16(1.0 - frac),
                jnp.where(spots == bf16(low + 1.0), bf16(frac), zero),
            )

        def high_of(row):
            return (spread(bins, row, 16) >> LO_BITS).astype(jnp.float32)

        def pair(i, carry):
            both = bf16(row_sums[pl.ds(aligned(i, 16), 16), :])
            left = bf16(jnp.where(upper, high_of(2 * i), -1.0))
            right = bf16(jnp.where(upper, -1.0, high_of(2 * i + 1)))
            lhs = []
            for h in range(HI):
                at = jnp.asarray(h, jnp.bfloat16)
                lhs.append(
                    jnp.concatenate(
                        [jnp.where(left == at, both, zero), jnp.where(right == at, both, zero)], axis=1
                    )
                )
            rhs = jnp.concatenate([weights_of(2 * i), weights_of(2 * i + 1)], axis=1)
            got = lax.dot_general(
                jnp.concatenate(lhs, axis=0), rhs, (((1,), (1,)), ((), ())), preferred_element_type=jnp.float32
            )
            got = jnp.concatenate([got, jnp.zeros((16 * HI, LANES - WIDE), jnp.float32)], axis=1)
            tiles = []
            carried = None
            for t in range(NBIN // LANES):
                even = got[32 * t : 32 * t + 16, :]
                odd = pltpu.roll(got[32 * t + 16 : 32 * t + 32, :], LO, 1)
                tile = even + jnp.where(lane >= LO, odd, 0.0)
                if carried is not None:
                    tile = tile + jnp.where(lane < LO, carried, 0.0)
                carried = odd
                tiles.append(tile)
            arrived[pl.ds(aligned(i, 16), 16), :] = bf16(jnp.concatenate(tiles, axis=1))
            return carry

        lax.fori_loop(low, high, pair, 0, unroll=UNROLL)

    def multiply(j, c0, c1):
        lhs = jnp.concatenate(
            [
                gains[j, pl.ds(pl.multiple_of((k * 4 + c1 * 2 + c0) * wide, 8), wide), :]
                for k in range(depth)
            ],
            axis=0,
        )
        return jnp.dot(lhs, arrived[...], preferred_element_type=jnp.float32)

    def stage_one(j, h, part):
        return pltpu.make_async_remote_copy(
            src_ref=first_out.at[j, h, part],
            dst_ref=first_in.at[j, h, part],
            send_sem=one_send.at[j, h, part],
            recv_sem=one_recv.at[j, h, part],
            device_id=(flips[h], q),
            device_id_type=MESH,
        )

    def stage_two(j, h):
        return pltpu.make_async_remote_copy(
            src_ref=second_out.at[j, h],
            dst_ref=second_in.at[j, h],
            send_sem=two_send.at[j, h],
            recv_sem=two_recv.at[j, h],
            device_id=(flips[1 - h], q),
            device_id_type=MESH,
        )

    def stage_three(j, i, to_z, to_q):
        return pltpu.make_async_remote_copy(
            src_ref=third_out.at[j, i],
            dst_ref=third_in.at[j, z * columns + q],
            send_sem=three_send.at[j, i],
            recv_sem=three_recv.at[j, z * columns + q],
            device_id=(to_z * 4 + corner, to_q),
            device_id_type=MESH,
        )

    def arrival(j, i):
        return pltpu.make_async_remote_copy(
            src_ref=third_out.at[j, i],
            dst_ref=third_in.at[j, i],
            send_sem=three_send.at[j, i],
            recv_sem=three_recv.at[j, i],
            device_id=((i // columns) * 4 + corner, lax.rem(i, columns)),
            device_id_type=MESH,
        )

    sides = (slice(0, half), slice(half, NBIN))

    def products(j):
        got = multiply(j, 1 - bit0, 1 - bit1)
        for h in range(2):
            first_out[j, h, 0] = bf16(got[:, sides[h]])
            stage_one(j, h, 0).start()
        got = multiply(j, 1 - bit0, bit1)
        first_out[j, 0, 1] = bf16(got[:, sides[0]])
        stage_one(j, 0, 1).start()
        kept[j, 1] = got[:, sides[1]]
        got = multiply(j, bit0, 1 - bit1)
        first_out[j, 1, 1] = bf16(got[:, sides[1]])
        stage_one(j, 1, 1).start()
        kept[j, 0] = got[:, sides[0]]
        got = multiply(j, bit0, bit1)
        for h in range(2):
            last[j, h] = got[:, sides[h]]

    def relay(from_g):
        posted_by(from_g).wait_recv()
        beside(lambda to_q: hand(from_g, to_q).start())

    ring(relay)

    def every(body):
        def one(i, c):
            body(i)
            return c

        lax.fori_loop(0, shards, one, 0)

    beside(lambda from_q: every(lambda from_g: handed_by(from_g, from_q).wait_recv()))
    slots = columns * shards * cap
    letters = got_in[...].reshape(slots, long + LANES)
    labels = letters[:, long:].astype(jnp.float32)[:, :1] - 1.0
    hot = bf16(
        (labels == lax.broadcasted_iota(jnp.int32, (slots, rows), 1).astype(jnp.float32)).astype(jnp.float32)
    )
    summed = lax.dot_general(
        hot, letters[:, :long], (((0,), (0,)), ((), ())), preferred_element_type=jnp.float32
    )
    for k in range(terms):
        row_sums[pl.ds(k, rows, stride=terms), :] = summed[:, k * panels : (k + 1) * panels]
    def second(j):
        for h in range(2):
            stage_one(j, h, 0).wait_recv()
            second_out[j, h] = bf16(kept[j, h] + first_in[j, h, 0].astype(jnp.float32))
            stage_two(j, h).start()

    def third(j):
        for h in range(2):
            stage_one(j, h, 1).wait_recv()
            stage_two(j, h).wait_recv()
            total = (
                last[j, h]
                + first_in[j, h, 1].astype(jnp.float32)
                + second_in[j, h].astype(jnp.float32)
            )
            third_out[j, :, :, sides[h]] = bf16(total).reshape(depth * columns, share, half)
        others(lambda i, to_z, to_q: stage_three(j, i, to_z, to_q).start())
        third_in[j, z * columns + q] = third_out[j, z * columns + q]

    pairs = rows // 2
    for j in range(per):
        if j == 0:
            scatter(j, 0, pairs)
        else:
            scatter(j, 0, pairs // 2)
            second(j - 1)
            scatter(j, pairs // 2, pairs)
        products(j)
        if j > 0:
            third(j - 1)
    second(per - 1)
    third(per - 1)
    for j in range(per):
        others(lambda i, to_z, to_q: arrival(j, i).wait_recv())
        for c in range(columns):
            total = third_in[j, c].astype(jnp.float32)
            for k in range(1, depth):
                total = total + third_in[j, k * columns + c].astype(jnp.float32)
            out_ref[:, c * per + j, :] = total
    for j in range(per):
        for h in range(2):
            for part in range(2):
                stage_one(j, h, part).wait_send()
            stage_two(j, h).wait_send()
        others(lambda i, to_z, to_q: stage_three(j, i, to_z, to_q).wait_send())
    ring(lambda to_g: post(to_g).wait_send())
    beside(lambda to_q: every(lambda from_g: hand(from_g, to_q).wait_send()))


def on_device(sources, owners, strip_rows, panel_counts, arrival_bins, arrival_fracs, gain_table):
    strips, terms, panels = sources.shape
    shards, columns = lax.axis_size("gx"), lax.axis_size("gy")
    cap = 2 * strips // shards
    rows, blocks = arrival_bins.shape[:2]
    observers = gain_table.shape[3]
    per = blocks // columns
    share = observers // (shards * columns)
    peers = shards // 4 * columns
    tall = peers * share
    half = NBIN // 2
    tiles_wide = observers // LANES
    wide = terms * panels + LANES
    assert panels == LANES and rows <= 256 and terms == 8
    flat = (
        gain_table.reshape(rows * terms, blocks, tiles_wide, LANES).transpose(0, 2, 1, 3).reshape(-1, LANES)
    )
    dma = pltpu.SemaphoreType.DMA
    return pl.pallas_call(
        functools.partial(signals_kernel, per, share, cap),
        out_shape=jax.ShapeDtypeStruct((share, blocks, NBIN), jnp.float32),
        in_specs=[pl.BlockSpec(memory_space=pltpu.VMEM)] * 4 + [pl.BlockSpec(memory_space=pl.ANY)] * 3,
        out_specs=pl.BlockSpec(memory_space=pltpu.VMEM),
        scratch_shapes=[
            pltpu.VMEM((per, observers, rows * terms), jnp.bfloat16),
            pltpu.VMEM((SLOTS, CHUNK * tiles_wide * blocks, LANES), jnp.bfloat16),
            pltpu.VMEM((per, CHUNK, observers), jnp.bfloat16),
            pltpu.VMEM((strips * terms, panels), jnp.float32),
            pltpu.VMEM((shards, cap, wide), jnp.bfloat16),
            pltpu.VMEM((columns, shards, cap, wide), jnp.bfloat16),
            pltpu.VMEM((rows * terms, panels), jnp.float32),
            pltpu.VMEM((rows * blocks, LANES), jnp.int32),
            pltpu.VMEM((rows * blocks, LANES), jnp.float32),
            pltpu.VMEM((rows * terms, NBIN), jnp.bfloat16),
            pltpu.VMEM((per, 2, 2, tall, half), jnp.bfloat16),
            pltpu.VMEM((per, 2, 2, tall, half), jnp.bfloat16),
            pltpu.VMEM((per, 2, tall, half), jnp.float32),
            pltpu.VMEM((per, 2, tall, half), jnp.float32),
            pltpu.VMEM((per, 2, tall, half), jnp.bfloat16),
            pltpu.VMEM((per, 2, tall, half), jnp.bfloat16),
            pltpu.VMEM((per, peers, share, NBIN), jnp.bfloat16),
            pltpu.VMEM((per, peers, share, NBIN), jnp.bfloat16),
            dma((SLOTS,)),
            dma((2,)),
            dma((shards,)),
            dma((shards,)),
            dma((columns, shards)),
            dma((columns, shards)),
            dma((per, 2, 2)),
            dma((per, 2, 2)),
            dma((per, 2)),
            dma((per, 2)),
            dma((per, peers)),
            dma((per, peers)),
        ],
        compiler_params=pltpu.CompilerParams(collective_id=0, has_side_effects=True),
        name="signals",
    )(
        sources,
        owners.reshape(1, strips),
        strip_rows.reshape(1, strips),
        panel_counts.reshape(1, strips),
        arrival_bins.reshape(-1, panels),
        arrival_fracs.reshape(-1, panels),
        flat,
    )


def solution(mesh):
    placed = (
        P(("gx", "gy"), None, None),
        P(("gx", "gy"), None),
        P(("gx", "gy")),
        P(("gx", "gy")),
        P("gx", None, None),
        P("gx", None, None),
        P("gx", None, None, None),
    )
    return jax.shard_map(
        on_device,
        mesh=mesh,
        in_specs=placed,
        out_specs=P(("gx", "gy"), None, None),
        check_vma=False,
    )
```

```python
import functools

import jax
import jax.numpy as jnp
from jax import lax
from jax.experimental import pallas as pl
from jax.experimental.pallas import tpu as pltpu
from jax.sharding import PartitionSpec as P

NBIN = 256
LANES = 128
LO = 64
LO_BITS = LO.bit_length() - 1
HI = NBIN // LO
WIDE = LO + 16
CHUNK = 128
SLOTS = 4
UNROLL = 64
CUTS = 2
MESH = pl.DeviceIdType.MESH


def bf16(v):
    return v.astype(jnp.bfloat16)


def aligned(i, n):
    return pl.multiple_of(i * n, n)


def signals_kernel(
    per, share, cap, sources_ref, owners_ref, strip_rows_ref, counts_ref,
    bins_hbm, fracs_hbm, gains_hbm, out_ref,
    gains, buffer, mixed, work, posted, got_in, row_sums,
    bins, fracs, arrived, first_out, first_in, kept, last, second_out, second_in, third_out, third_in,
    gain_sems, table_sems, post_send, post_recv, pass_send, pass_recv,
    one_send, one_recv, two_send, two_recv, three_send, three_recv,
):
    g = lax.axis_index("gx")
    q = lax.axis_index("gy")
    shards = lax.axis_size("gx")
    columns = lax.axis_size("gy")
    depth = shards // 4
    bit0, bit1, z = lax.rem(g, 2), lax.rem(g // 2, 2), g // 4
    flips = (g + 1 - 2 * bit0, g + 2 - 4 * bit1)
    corner = lax.rem(g, 4)
    rows = row_sums.shape[0] // 8
    wide = columns * share // CUTS
    tall = depth * wide
    half = NBIN // 2

    observers = gains.shape[1]
    tiles_wide = observers // LANES
    blocks = per * columns
    deep = tiles_wide * blocks
    group = 256 // deep
    steps = gains.shape[2] // CHUNK
    size = CHUNK * deep

    def fetch(i):
        slot = lax.rem(i, SLOTS)
        return pltpu.make_async_copy(
            gains_hbm.at[pl.ds(aligned(i, size), size)], buffer.at[slot], gain_sems.at[slot]
        )

    for i in range(SLOTS - 1):
        fetch(i).start()
    tables = (
        pltpu.make_async_copy(bins_hbm, bins, table_sems.at[0]),
        pltpu.make_async_copy(fracs_hbm, fracs, table_sems.at[1]),
    )
    for table in tables:
        table.start()

    barrier = pltpu.get_barrier_semaphore()

    def greet(to_g, to_q):
        pl.semaphore_signal(barrier, inc=1, device_id=(to_g, to_q), device_id_type=MESH)

    def ring(body):
        def one(i, c):
            body(lax.rem(g + i, shards))
            return c

        lax.fori_loop(1, shards, one, 0)

    ring(lambda to_g: greet(to_g, q))

    def beside(body):
        def one(i, c):
            body(lax.rem(q + i, columns))
            return c

        lax.fori_loop(1, columns, one, 0)

    def greet_column(to_q):
        def one(k, c):
            greet(k * 4 + corner, to_q)
            return c

        lax.fori_loop(0, depth, one, 0)

    beside(greet_column)

    strips, terms, panels = sources_ref.shape
    long = terms * panels
    work[...] = sources_ref[...].reshape(strips * terms, panels).astype(jnp.float32)
    before = lax.broadcasted_iota(jnp.int32, (strips, strips), 1) < lax.broadcasted_iota(
        jnp.int32, (strips, strips), 0
    )
    eye = lax.broadcasted_iota(jnp.int32, (strips, strips), 1) == lax.broadcasted_iota(
        jnp.int32, (strips, strips), 0
    )

    def stood(ref):
        row = ref[...].astype(jnp.float32)
        return jnp.sum(jnp.where(eye, jnp.broadcast_to(row, eye.shape), 0.0), axis=1, keepdims=True)

    targets = stood(owners_ref)
    same = jnp.logical_and(targets == owners_ref[...].astype(jnp.float32), before)
    order = jnp.sum(same.astype(jnp.float32), axis=1, keepdims=True)
    spot_of = (targets * cap + order).astype(jnp.int32)
    placing = bf16(
        (spot_of == lax.broadcasted_iota(jnp.int32, (strips, shards * cap), 1)).astype(jnp.float32)
    )
    live = lax.broadcasted_iota(jnp.int32, (strips, panels), 1).astype(jnp.float32) < stood(counts_ref)
    pieces = [
        bf16(jnp.where(live, work[pl.ds(k, strips, stride=terms), :], 0.0)) for k in range(terms)
    ]
    labels = stood(strip_rows_ref) + 1.0
    pieces.append(
        bf16(jnp.where(lax.broadcasted_iota(jnp.int32, (strips, LANES), 1) == 0, labels, 0.0))
    )
    placed = bf16(
        lax.dot_general(
            placing,
            jnp.concatenate(pieces, axis=1),
            (((0,), (0,)), ((), ())),
            preferred_element_type=jnp.float32,
        )
    )
    posted[...] = placed.reshape(shards, cap, long + LANES)

    def post(to_g):
        return pltpu.make_async_remote_copy(
            src_ref=posted.at[to_g],
            dst_ref=got_in.at[q, g],
            send_sem=post_send.at[to_g],
            recv_sem=post_recv.at[g],
            device_id=(to_g, q),
            device_id_type=MESH,
        )

    def posted_by(from_g):
        return pltpu.make_async_remote_copy(
            src_ref=posted.at[from_g],
            dst_ref=got_in.at[q, from_g],
            send_sem=post_send.at[from_g],
            recv_sem=post_recv.at[from_g],
            device_id=(from_g, q),
            device_id_type=MESH,
        )

    def hand(from_g, to_q):
        return pltpu.make_async_remote_copy(
            src_ref=got_in.at[q, from_g],
            dst_ref=got_in.at[q, from_g],
            send_sem=pass_send.at[to_q, from_g],
            recv_sem=pass_recv.at[q, from_g],
            device_id=(g, to_q),
            device_id_type=MESH,
        )

    def handed_by(from_g, from_q):
        return pltpu.make_async_remote_copy(
            src_ref=got_in.at[from_q, from_g],
            dst_ref=got_in.at[from_q, from_g],
            send_sem=pass_send.at[from_q, from_g],
            recv_sem=pass_recv.at[from_q, from_g],
            device_id=(g, from_q),
            device_id_type=MESH,
        )

    height = per * tiles_wide * group
    row = lax.broadcasted_iota(jnp.int32, (height, 256), 0)
    spot = lax.broadcasted_iota(jnp.int32, (height, 256), 1)
    wanted = (
        lax.rem(row, group) * deep
        + lax.rem(row // group, tiles_wide) * blocks
        + q * per
        + row // (group * tiles_wide)
    )
    pick = bf16((wanted == spot).astype(jnp.float32))

    def turn(i, carry):
        slot = lax.rem(i, SLOTS)

        @pl.when(i + SLOTS - 1 < steps)
        def _():
            fetch(i + SLOTS - 1).start()

        fetch(i).wait()

        def part(j, c):
            one = buffer[slot, pl.ds(aligned(j, 512), 256), :]
            two = buffer[slot, pl.ds(aligned(j, 512) + 256, 256), :]
            got = jnp.dot(
                pick, jnp.concatenate([one, two], axis=1), preferred_element_type=jnp.float32
            )
            for o in range(per):
                for t in range(tiles_wide):
                    at = (o * tiles_wide + t) * group
                    both = jnp.concatenate(
                        [got[at : at + group, :LANES], got[at : at + group, LANES:]], axis=0
                    )
                    mixed[
                        o, pl.ds(aligned(j, 2 * group), 2 * group), t * LANES : (t + 1) * LANES
                    ] = bf16(both)
            return c

        lax.fori_loop(0, CHUNK // (2 * group), part, 0, unroll=True)
        for o in range(per):
            for t in range(tiles_wide):
                gains[o, t * LANES : (t + 1) * LANES, pl.ds(aligned(i, CHUNK), CHUNK)] = mixed[
                    o, :, t * LANES : (t + 1) * LANES
                ].T
        return carry

    pl.semaphore_wait(barrier, shards - 1 + depth * (columns - 1))
    turn_round = jnp.where(z * 2 < depth, shards - 1, 1)

    def far_first(i, c):
        post(lax.rem(g + i * turn_round, shards)).start()
        return c

    lax.fori_loop(1, shards, far_first, 0)
    got_in[q, g] = posted[g]
    beside(lambda to_q: hand(g, to_q).start())

    lax.fori_loop(0, steps, turn, 0)
    for table in tables:
        table.wait()

    spots = bf16(lax.broadcasted_iota(jnp.int32, (WIDE, LANES), 0).astype(jnp.float32))
    lane = lax.broadcasted_iota(jnp.int32, (16, LANES), 1)
    upper = lax.broadcasted_iota(jnp.int32, (16, LANES), 0) < 8
    zero = jnp.zeros((), jnp.bfloat16)

    def scatter(j, low, high):
        block = q * per + j

        def spread(ref, row, n):
            return jnp.broadcast_to(ref[pl.ds(row * blocks + block, 1), :], (n, LANES))

        def weights_of(row):
            frac = spread(fracs, row, WIDE)
            low = (spread(bins, row, WIDE) & (LO - 1)).astype(jnp.float32)
            return jnp.where(
                spots == bf16(low),
                bf16(1.0 - frac),
                jnp.where(spots == bf16(low + 1.0), bf16(frac), zero),
            )

        def high_of(row):
            return (spread(bins, row, 16) >> LO_BITS).astype(jnp.float32)

        def pair(i, carry):
            both = bf16(row_sums[pl.ds(aligned(i, 16), 16), :])
            left = bf16(jnp.where(upper, high_of(2 * i), -1.0))
            right = bf16(jnp.where(upper, -1.0, high_of(2 * i + 1)))
            lhs = []
            for h in range(HI):
                at = jnp.asarray(h, jnp.bfloat16)
                lhs.append(
                    jnp.concatenate(
                        [jnp.where(left == at, both, zero), jnp.where(right == at, both, zero)], axis=1
                    )
                )
            rhs = jnp.concatenate([weights_of(2 * i), weights_of(2 * i + 1)], axis=1)
            got = lax.dot_general(
                jnp.concatenate(lhs, axis=0), rhs, (((1,), (1,)), ((), ())), preferred_element_type=jnp.float32
            )
            got = jnp.concatenate([got, jnp.zeros((16 * HI, LANES - WIDE), jnp.float32)], axis=1)
            tiles = []
            carried = None
            for t in range(NBIN // LANES):
                even = got[32 * t : 32 * t + 16, :]
                odd = pltpu.roll(got[32 * t + 16 : 32 * t + 32, :], LO, 1)
                tile = even + jnp.where(lane >= LO, odd, 0.0)
                if carried is not None:
                    tile = tile + jnp.where(lane < LO, carried, 0.0)
                carried = odd
                tiles.append(tile)
            arrived[pl.ds(aligned(i, 16), 16), :] = bf16(jnp.concatenate(tiles, axis=1))
            return carry

        lax.fori_loop(low, high, pair, 0, unroll=UNROLL)

    def multiply(j, u, c0, c1):
        lhs = jnp.concatenate(
            [
                gains[j, pl.ds(pl.multiple_of((k * 4 + c1 * 2 + c0) * wide * CUTS + u * wide, 8), wide), :]
                for k in range(depth)
            ],
            axis=0,
        )
        return jnp.dot(lhs, arrived[...], preferred_element_type=jnp.float32)

    def stage_one(j, u, h, part):
        return pltpu.make_async_remote_copy(
            src_ref=first_out.at[j, u, h, part],
            dst_ref=first_in.at[j, u, h, part],
            send_sem=one_send.at[j, u, h, part],
            recv_sem=one_recv.at[j, u, h, part],
            device_id=(flips[h], q),
            device_id_type=MESH,
        )

    def stage_two(j, u, h):
        return pltpu.make_async_remote_copy(
            src_ref=second_out.at[j, u, h],
            dst_ref=second_in.at[j, u, h],
            send_sem=two_send.at[j, u, h],
            recv_sem=two_recv.at[j, u, h],
            device_id=(flips[1 - h], q),
            device_id_type=MESH,
        )

    def stage_three(j, to_z, to_q):
        return pltpu.make_async_remote_copy(
            src_ref=third_out.at[j, to_z, to_q],
            dst_ref=third_in.at[j, z, q],
            send_sem=three_send.at[j, to_z, to_q],
            recv_sem=three_recv.at[j, z, q],
            device_id=(to_z * 4 + corner, to_q),
            device_id_type=MESH,
        )

    def arrival(j, from_z, from_q):
        return pltpu.make_async_remote_copy(
            src_ref=third_out.at[j, from_z, from_q],
            dst_ref=third_in.at[j, from_z, from_q],
            send_sem=three_send.at[j, from_z, from_q],
            recv_sem=three_recv.at[j, from_z, from_q],
            device_id=(from_z * 4 + corner, from_q),
            device_id_type=MESH,
        )

    def others(body, low, high):
        count = high - low

        def one(n, c):
            to_z = lax.rem(z + jnp.where(z * 2 < depth, 2 * depth - 1 - n // count, 1 + n // count), depth)
            to_q = low + lax.rem(n, count)

            @pl.when(jnp.logical_or(to_z != z, to_q != q))
            def _():
                body(to_z, to_q)

            return c

        lax.fori_loop(0, depth * count, one, 0)

    sides = (slice(0, half), slice(half, NBIN))
    span = columns // CUTS

    def products(j, u):
        got = multiply(j, u, 1 - bit0, 1 - bit1)
        for h in range(2):
            first_out[j, u, h, 0] = bf16(got[:, sides[h]])
            stage_one(j, u, h, 0).start()
        got = multiply(j, u, 1 - bit0, bit1)
        first_out[j, u, 0, 1] = bf16(got[:, sides[0]])
        stage_one(j, u, 0, 1).start()
        kept[j, u, 1] = got[:, sides[1]]
        got = multiply(j, u, bit0, 1 - bit1)
        first_out[j, u, 1, 1] = bf16(got[:, sides[1]])
        stage_one(j, u, 1, 1).start()
        kept[j, u, 0] = got[:, sides[0]]
        got = multiply(j, u, bit0, bit1)
        for h in range(2):
            last[j, u, h] = got[:, sides[h]]

    def second(j, u):
        for h in range(2):
            stage_one(j, u, h, 0).wait_recv()
            second_out[j, u, h] = bf16(kept[j, u, h] + first_in[j, u, h, 0].astype(jnp.float32))
            stage_two(j, u, h).start()

    def third(j, u):
        for h in range(2):
            stage_one(j, u, h, 1).wait_recv()
            stage_two(j, u, h).wait_recv()
            total = (
                last[j, u, h]
                + first_in[j, u, h, 1].astype(jnp.float32)
                + second_in[j, u, h].astype(jnp.float32)
            )
            third_out[j, :, u * span : (u + 1) * span, :, sides[h]] = bf16(total).reshape(
                depth, span, share, half
            )
        others(lambda to_z, to_q: stage_three(j, to_z, to_q).start(), u * span, (u + 1) * span)

    def relay(from_g):
        posted_by(from_g).wait_recv()
        beside(lambda to_q: hand(from_g, to_q).start())

    ring(relay)

    def every(body):
        def one(i, c):
            body(i)
            return c

        lax.fori_loop(0, shards, one, 0)

    beside(lambda from_q: every(lambda from_g: handed_by(from_g, from_q).wait_recv()))
    slots = columns * shards * cap
    letters = got_in[...].reshape(slots, long + LANES)
    labels = letters[:, long:].astype(jnp.float32)[:, :1] - 1.0
    hot = bf16(
        (labels == lax.broadcasted_iota(jnp.int32, (slots, rows), 1).astype(jnp.float32)).astype(jnp.float32)
    )
    summed = lax.dot_general(
        hot, letters[:, :long], (((0,), (0,)), ((), ())), preferred_element_type=jnp.float32
    )
    for k in range(terms):
        row_sums[pl.ds(k, rows, stride=terms), :] = summed[:, k * panels : (k + 1) * panels]
    pairs = rows // 2
    for j in range(per):
        if j == 0:
            scatter(j, 0, pairs)
        else:
            scatter(j, 0, pairs // 2)
            second(j - 1, 0)
            scatter(j, pairs // 2, pairs)
            for u in range(1, CUTS):
                second(j - 1, u)
        for u in range(CUTS):
            products(j, u)
            if j > 0:
                third(j - 1, u)
    for u in range(CUTS):
        second(per - 1, u)
    for u in range(CUTS):
        third(per - 1, u)
    for j in range(per):
        third_in[j, z, q] = third_out[j, z, q]
    for j in range(per):
        others(lambda from_z, from_q: arrival(j, from_z, from_q).wait_recv(), 0, columns)
        for c in range(columns):
            total = third_in[j, 0, c].astype(jnp.float32)
            for k in range(1, depth):
                total = total + third_in[j, k, c].astype(jnp.float32)
            out_ref[:, c * per + j, :] = total
    for j in range(per):
        for u in range(CUTS):
            for h in range(2):
                for part in range(2):
                    stage_one(j, u, h, part).wait_send()
                stage_two(j, u, h).wait_send()
        others(lambda to_z, to_q: stage_three(j, to_z, to_q).wait_send(), 0, columns)
    ring(lambda to_g: post(to_g).wait_send())
    beside(lambda to_q: every(lambda from_g: hand(from_g, to_q).wait_send()))


def on_device(sources, owners, strip_rows, panel_counts, arrival_bins, arrival_fracs, gain_table):
    strips, terms, panels = sources.shape
    shards, columns = lax.axis_size("gx"), lax.axis_size("gy")
    cap = 2 * strips // shards
    rows, blocks = arrival_bins.shape[:2]
    observers = gain_table.shape[3]
    per = blocks // columns
    share = observers // (shards * columns)
    depth = shards // 4
    tall = depth * columns * share // CUTS
    half = NBIN // 2
    tiles_wide = observers // LANES
    wide = terms * panels + LANES
    assert panels == LANES and rows <= 256 and terms == 8
    flat = (
        gain_table.reshape(rows * terms, blocks, tiles_wide, LANES).transpose(0, 2, 1, 3).reshape(-1, LANES)
    )
    dma = pltpu.SemaphoreType.DMA
    return pl.pallas_call(
        functools.partial(signals_kernel, per, share, cap),
        out_shape=jax.ShapeDtypeStruct((share, blocks, NBIN), jnp.float32),
        in_specs=[pl.BlockSpec(memory_space=pltpu.VMEM)] * 4 + [pl.BlockSpec(memory_space=pl.ANY)] * 3,
        out_specs=pl.BlockSpec(memory_space=pltpu.VMEM),
        scratch_shapes=[
            pltpu.VMEM((per, observers, rows * terms), jnp.bfloat16),
            pltpu.VMEM((SLOTS, CHUNK * tiles_wide * blocks, LANES), jnp.bfloat16),
            pltpu.VMEM((per, CHUNK, observers), jnp.bfloat16),
            pltpu.VMEM((strips * terms, panels), jnp.float32),
            pltpu.VMEM((shards, cap, wide), jnp.bfloat16),
            pltpu.VMEM((columns, shards, cap, wide), jnp.bfloat16),
            pltpu.VMEM((rows * terms, panels), jnp.float32),
            pltpu.VMEM((rows * blocks, LANES), jnp.int32),
            pltpu.VMEM((rows * blocks, LANES), jnp.float32),
            pltpu.VMEM((rows * terms, NBIN), jnp.bfloat16),
            pltpu.VMEM((per, CUTS, 2, 2, tall, half), jnp.bfloat16),
            pltpu.VMEM((per, CUTS, 2, 2, tall, half), jnp.bfloat16),
            pltpu.VMEM((per, CUTS, 2, tall, half), jnp.float32),
            pltpu.VMEM((per, CUTS, 2, tall, half), jnp.float32),
            pltpu.VMEM((per, CUTS, 2, tall, half), jnp.bfloat16),
            pltpu.VMEM((per, CUTS, 2, tall, half), jnp.bfloat16),
            pltpu.VMEM((per, depth, columns, share, NBIN), jnp.bfloat16),
            pltpu.VMEM((per, depth, columns, share, NBIN), jnp.bfloat16),
            dma((SLOTS,)),
            dma((2,)),
            dma((shards,)),
            dma((shards,)),
            dma((columns, shards)),
            dma((columns, shards)),
            dma((per, CUTS, 2, 2)),
            dma((per, CUTS, 2, 2)),
            dma((per, CUTS, 2)),
            dma((per, CUTS, 2)),
            dma((per, depth, columns)),
            dma((per, depth, columns)),
        ],
        compiler_params=pltpu.CompilerParams(collective_id=0, has_side_effects=True),
        name="signals",
    )(
        sources,
        owners.reshape(1, strips),
        strip_rows.reshape(1, strips),
        panel_counts.reshape(1, strips),
        arrival_bins.reshape(-1, panels),
        arrival_fracs.reshape(-1, panels),
        flat,
    )


def solution(mesh):
    placed = (
        P(("gx", "gy"), None, None),
        P(("gx", "gy"), None),
        P(("gx", "gy")),
        P(("gx", "gy")),
        P("gx", None, None),
        P("gx", None, None),
        P("gx", None, None, None),
    )
    return jax.shard_map(
        on_device,
        mesh=mesh,
        in_specs=placed,
        out_specs=P(("gx", "gy"), None, None),
        check_vma=False,
    )
```

```python
import functools

import jax
import jax.numpy as jnp
from jax import lax
from jax.experimental import pallas as pl
from jax.experimental.pallas import tpu as pltpu
from jax.sharding import PartitionSpec as P

NBIN = 256
LANES = 128
LO = 64
LO_BITS = LO.bit_length() - 1
HI = NBIN // LO
WIDE = LO + 16
CHUNK = 256
SLOTS = 4
UNROLL = 64
CUTS = 2
MESH = pl.DeviceIdType.MESH


def bf16(v):
    return v.astype(jnp.bfloat16)


def aligned(i, n):
    return pl.multiple_of(i * n, n)


def signals_kernel(
    per, share, cap, sources_ref, owners_ref, strip_rows_ref, counts_ref,
    bins_hbm, fracs_hbm, gains_hbm, out_ref,
    gains, buffer, mixed, work, posted, got_in, row_sums,
    bins, fracs, arrived, first_out, first_in, kept, last, second_out, second_in, third_out, third_in,
    gain_sems, table_sems, post_send, post_recv, pass_send, pass_recv,
    one_send, one_recv, two_send, two_recv, three_send, three_recv,
):
    g = lax.axis_index("gx")
    q = lax.axis_index("gy")
    shards = lax.axis_size("gx")
    columns = lax.axis_size("gy")
    depth = shards // 4
    bit0, bit1, z = lax.rem(g, 2), lax.rem(g // 2, 2), g // 4
    flips = (g + 1 - 2 * bit0, g + 2 - 4 * bit1)
    corner = lax.rem(g, 4)
    rows = row_sums.shape[0] // 8
    wide = columns * share // CUTS
    tall = depth * wide
    half = NBIN // 2

    observers = gains.shape[1]
    tiles_wide = observers // LANES
    blocks = per * columns
    deep = tiles_wide * blocks
    group = 256 // deep
    steps = gains.shape[2] // CHUNK
    size = CHUNK * deep

    def fetch(i):
        slot = lax.rem(i, SLOTS)
        return pltpu.make_async_copy(
            gains_hbm.at[pl.ds(aligned(i, size), size)], buffer.at[slot], gain_sems.at[slot]
        )

    for i in range(SLOTS - 1):
        fetch(i).start()
    tables = (
        pltpu.make_async_copy(bins_hbm, bins, table_sems.at[0]),
        pltpu.make_async_copy(fracs_hbm, fracs, table_sems.at[1]),
    )
    for table in tables:
        table.start()

    barrier = pltpu.get_barrier_semaphore()

    def greet(to_g, to_q):
        pl.semaphore_signal(barrier, inc=1, device_id=(to_g, to_q), device_id_type=MESH)

    def ring(body):
        def one(i, c):
            body(lax.rem(g + i, shards))
            return c

        lax.fori_loop(1, shards, one, 0)

    ring(lambda to_g: greet(to_g, q))

    def beside(body):
        def one(i, c):
            body(lax.rem(q + i, columns))
            return c

        lax.fori_loop(1, columns, one, 0)

    def greet_column(to_q):
        def one(k, c):
            greet(k * 4 + corner, to_q)
            return c

        lax.fori_loop(0, depth, one, 0)

    beside(greet_column)

    strips, terms, panels = sources_ref.shape
    long = terms * panels
    work[...] = sources_ref[...].reshape(strips * terms, panels).astype(jnp.float32)
    before = lax.broadcasted_iota(jnp.int32, (strips, strips), 1) < lax.broadcasted_iota(
        jnp.int32, (strips, strips), 0
    )
    eye = lax.broadcasted_iota(jnp.int32, (strips, strips), 1) == lax.broadcasted_iota(
        jnp.int32, (strips, strips), 0
    )

    def stood(ref):
        row = ref[...].astype(jnp.float32)
        return jnp.sum(jnp.where(eye, jnp.broadcast_to(row, eye.shape), 0.0), axis=1, keepdims=True)

    targets = stood(owners_ref)
    same = jnp.logical_and(targets == owners_ref[...].astype(jnp.float32), before)
    order = jnp.sum(same.astype(jnp.float32), axis=1, keepdims=True)
    spot_of = (targets * cap + order).astype(jnp.int32)
    placing = bf16(
        (spot_of == lax.broadcasted_iota(jnp.int32, (strips, shards * cap), 1)).astype(jnp.float32)
    )
    live = lax.broadcasted_iota(jnp.int32, (strips, panels), 1).astype(jnp.float32) < stood(counts_ref)
    pieces = [
        bf16(jnp.where(live, work[pl.ds(k, strips, stride=terms), :], 0.0)) for k in range(terms)
    ]
    labels = stood(strip_rows_ref) + 1.0
    pieces.append(
        bf16(jnp.where(lax.broadcasted_iota(jnp.int32, (strips, LANES), 1) == 0, labels, 0.0))
    )
    placed = bf16(
        lax.dot_general(
            placing,
            jnp.concatenate(pieces, axis=1),
            (((0,), (0,)), ((), ())),
            preferred_element_type=jnp.float32,
        )
    )
    posted[...] = placed.reshape(shards, cap, long + LANES)

    def post(to_g):
        return pltpu.make_async_remote_copy(
            src_ref=posted.at[to_g],
            dst_ref=got_in.at[q, g],
            send_sem=post_send.at[to_g],
            recv_sem=post_recv.at[g],
            device_id=(to_g, q),
            device_id_type=MESH,
        )

    def posted_by(from_g):
        return pltpu.make_async_remote_copy(
            src_ref=posted.at[from_g],
            dst_ref=got_in.at[q, from_g],
            send_sem=post_send.at[from_g],
            recv_sem=post_recv.at[from_g],
            device_id=(from_g, q),
            device_id_type=MESH,
        )

    def hand(from_g, to_q):
        return pltpu.make_async_remote_copy(
            src_ref=got_in.at[q, from_g],
            dst_ref=got_in.at[q, from_g],
            send_sem=pass_send.at[to_q, from_g],
            recv_sem=pass_recv.at[q, from_g],
            device_id=(g, to_q),
            device_id_type=MESH,
        )

    def handed_by(from_g, from_q):
        return pltpu.make_async_remote_copy(
            src_ref=got_in.at[from_q, from_g],
            dst_ref=got_in.at[from_q, from_g],
            send_sem=pass_send.at[from_q, from_g],
            recv_sem=pass_recv.at[from_q, from_g],
            device_id=(g, from_q),
            device_id_type=MESH,
        )

    height = per * tiles_wide * group
    row = lax.broadcasted_iota(jnp.int32, (height, 256), 0)
    spot = lax.broadcasted_iota(jnp.int32, (height, 256), 1)
    wanted = (
        lax.rem(row, group) * deep
        + lax.rem(row // group, tiles_wide) * blocks
        + q * per
        + row // (group * tiles_wide)
    )
    pick = bf16((wanted == spot).astype(jnp.float32))

    def turn(i, carry):
        slot = lax.rem(i, SLOTS)

        @pl.when(i + SLOTS - 1 < steps)
        def _():
            fetch(i + SLOTS - 1).start()

        fetch(i).wait()

        def part(j, c):
            one = buffer[slot, pl.ds(aligned(j, 512), 256), :]
            two = buffer[slot, pl.ds(aligned(j, 512) + 256, 256), :]
            got = jnp.dot(
                pick, jnp.concatenate([one, two], axis=1), preferred_element_type=jnp.float32
            )
            for o in range(per):
                for t in range(tiles_wide):
                    at = (o * tiles_wide + t) * group
                    both = jnp.concatenate(
                        [got[at : at + group, :LANES], got[at : at + group, LANES:]], axis=0
                    )
                    mixed[
                        o, pl.ds(aligned(j, 2 * group), 2 * group), t * LANES : (t + 1) * LANES
                    ] = bf16(both)
            return c

        lax.fori_loop(0, CHUNK // (2 * group), part, 0, unroll=True)
        for o in range(per):
            for t in range(tiles_wide):
                gains[o, t * LANES : (t + 1) * LANES, pl.ds(aligned(i, CHUNK), CHUNK)] = mixed[
                    o, :, t * LANES : (t + 1) * LANES
                ].T
        return carry

    pl.semaphore_wait(barrier, shards - 1 + depth * (columns - 1))
    turn_round = jnp.where(z * 2 < depth, shards - 1, 1)

    def far_first(i, c):
        post(lax.rem(g + i * turn_round, shards)).start()
        return c

    lax.fori_loop(1, shards, far_first, 0)
    got_in[q, g] = posted[g]
    beside(lambda to_q: hand(g, to_q).start())

    lax.fori_loop(0, steps, turn, 0)
    for table in tables:
        table.wait()

    spots = bf16(lax.broadcasted_iota(jnp.int32, (WIDE, LANES), 0).astype(jnp.float32))
    lane = lax.broadcasted_iota(jnp.int32, (16, LANES), 1)
    upper = lax.broadcasted_iota(jnp.int32, (16, LANES), 0) < 8
    zero = jnp.zeros((), jnp.bfloat16)

    def scatter(j, low, high):
        block = q * per + j

        def spread(ref, row, n):
            return jnp.broadcast_to(ref[pl.ds(row * blocks + block, 1), :], (n, LANES))

        def weights_of(row):
            frac = spread(fracs, row, WIDE)
            low = (spread(bins, row, WIDE) & (LO - 1)).astype(jnp.float32)
            return jnp.where(
                spots == bf16(low),
                bf16(1.0 - frac),
                jnp.where(spots == bf16(low + 1.0), bf16(frac), zero),
            )

        def high_of(row):
            return (spread(bins, row, 16) >> LO_BITS).astype(jnp.float32)

        def pair(i, carry):
            both = bf16(row_sums[pl.ds(aligned(i, 16), 16), :])
            left = bf16(jnp.where(upper, high_of(2 * i), -1.0))
            right = bf16(jnp.where(upper, -1.0, high_of(2 * i + 1)))
            lhs = []
            for h in range(HI):
                at = jnp.asarray(h, jnp.bfloat16)
                lhs.append(
                    jnp.concatenate(
                        [jnp.where(left == at, both, zero), jnp.where(right == at, both, zero)], axis=1
                    )
                )
            rhs = jnp.concatenate([weights_of(2 * i), weights_of(2 * i + 1)], axis=1)
            got = lax.dot_general(
                jnp.concatenate(lhs, axis=0), rhs, (((1,), (1,)), ((), ())), preferred_element_type=jnp.float32
            )
            got = jnp.concatenate([got, jnp.zeros((16 * HI, LANES - WIDE), jnp.float32)], axis=1)
            tiles = []
            carried = None
            for t in range(NBIN // LANES):
                even = got[32 * t : 32 * t + 16, :]
                odd = pltpu.roll(got[32 * t + 16 : 32 * t + 32, :], LO, 1)
                tile = even + jnp.where(lane >= LO, odd, 0.0)
                if carried is not None:
                    tile = tile + jnp.where(lane < LO, carried, 0.0)
                carried = odd
                tiles.append(tile)
            arrived[pl.ds(aligned(i, 16), 16), :] = bf16(jnp.concatenate(tiles, axis=1))
            return carry

        lax.fori_loop(low, high, pair, 0, unroll=UNROLL)

    def multiply(j, u, c0, c1):
        lhs = jnp.concatenate(
            [
                gains[j, pl.ds(pl.multiple_of((k * 4 + c1 * 2 + c0) * wide * CUTS + u * wide, 8), wide), :]
                for k in range(depth)
            ],
            axis=0,
        )
        return jnp.dot(lhs, arrived[...], preferred_element_type=jnp.float32)

    def stage_one(j, u, h, part):
        return pltpu.make_async_remote_copy(
            src_ref=first_out.at[j, u, h, part],
            dst_ref=first_in.at[j, u, h, part],
            send_sem=one_send.at[j, u, h, part],
            recv_sem=one_recv.at[j, u, h, part],
            device_id=(flips[h], q),
            device_id_type=MESH,
        )

    def stage_two(j, u, h):
        return pltpu.make_async_remote_copy(
            src_ref=second_out.at[j, u, h],
            dst_ref=second_in.at[j, u, h],
            send_sem=two_send.at[j, u, h],
            recv_sem=two_recv.at[j, u, h],
            device_id=(flips[1 - h], q),
            device_id_type=MESH,
        )

    def stage_three(j, to_z, to_q):
        return pltpu.make_async_remote_copy(
            src_ref=third_out.at[j, to_z, to_q],
            dst_ref=third_in.at[j, z, q],
            send_sem=three_send.at[j, to_z, to_q],
            recv_sem=three_recv.at[j, z, q],
            device_id=(to_z * 4 + corner, to_q),
            device_id_type=MESH,
        )

    def arrival(j, from_z, from_q):
        return pltpu.make_async_remote_copy(
            src_ref=third_out.at[j, from_z, from_q],
            dst_ref=third_in.at[j, from_z, from_q],
            send_sem=three_send.at[j, from_z, from_q],
            recv_sem=three_recv.at[j, from_z, from_q],
            device_id=(from_z * 4 + corner, from_q),
            device_id_type=MESH,
        )

    def others(body, low, high):
        count = high - low

        def one(n, c):
            to_z = lax.rem(z + jnp.where(z * 2 < depth, 2 * depth - 1 - n // count, 1 + n // count), depth)
            to_q = low + lax.rem(n, count)

            @pl.when(jnp.logical_or(to_z != z, to_q != q))
            def _():
                body(to_z, to_q)

            return c

        lax.fori_loop(0, depth * count, one, 0)

    sides = (slice(0, half), slice(half, NBIN))
    span = columns // CUTS

    def products(j, u):
        got = multiply(j, u, 1 - bit0, 1 - bit1)
        for h in range(2):
            first_out[j, u, h, 0] = bf16(got[:, sides[h]])
            stage_one(j, u, h, 0).start()
        got = multiply(j, u, 1 - bit0, bit1)
        first_out[j, u, 0, 1] = bf16(got[:, sides[0]])
        stage_one(j, u, 0, 1).start()
        kept[j, u, 1] = got[:, sides[1]]
        got = multiply(j, u, bit0, 1 - bit1)
        first_out[j, u, 1, 1] = bf16(got[:, sides[1]])
        stage_one(j, u, 1, 1).start()
        kept[j, u, 0] = got[:, sides[0]]
        got = multiply(j, u, bit0, bit1)
        for h in range(2):
            last[j, u, h] = got[:, sides[h]]

    def second(j, u):
        for h in range(2):
            stage_one(j, u, h, 0).wait_recv()
            second_out[j, u, h] = bf16(kept[j, u, h] + first_in[j, u, h, 0].astype(jnp.float32))
            stage_two(j, u, h).start()

    def third(j, u):
        for h in range(2):
            stage_one(j, u, h, 1).wait_recv()
            stage_two(j, u, h).wait_recv()
            total = (
                last[j, u, h]
                + first_in[j, u, h, 1].astype(jnp.float32)
                + second_in[j, u, h].astype(jnp.float32)
            )
            third_out[j, :, u * span : (u + 1) * span, :, sides[h]] = bf16(total).reshape(
                depth, span, share, half
            )
        others(lambda to_z, to_q: stage_three(j, to_z, to_q).start(), u * span, (u + 1) * span)

    def relay(from_g):
        posted_by(from_g).wait_recv()
        beside(lambda to_q: hand(from_g, to_q).start())

    ring(relay)

    def every(body):
        def one(i, c):
            body(i)
            return c

        lax.fori_loop(0, shards, one, 0)

    beside(lambda from_q: every(lambda from_g: handed_by(from_g, from_q).wait_recv()))
    slots = columns * shards * cap
    letters = got_in[...].reshape(slots, long + LANES)
    labels = letters[:, long:].astype(jnp.float32)[:, :1] - 1.0
    hot = bf16(
        (labels == lax.broadcasted_iota(jnp.int32, (slots, rows), 1).astype(jnp.float32)).astype(jnp.float32)
    )
    summed = lax.dot_general(
        hot, letters[:, :long], (((0,), (0,)), ((), ())), preferred_element_type=jnp.float32
    )
    for k in range(terms):
        row_sums[pl.ds(k, rows, stride=terms), :] = summed[:, k * panels : (k + 1) * panels]
    pairs = rows // 2
    for j in range(per):
        if j == 0:
            scatter(j, 0, pairs)
        else:
            scatter(j, 0, pairs // 2)
            second(j - 1, 0)
            scatter(j, pairs // 2, pairs)
            for u in range(1, CUTS):
                second(j - 1, u)
        for u in range(CUTS):
            products(j, u)
            if j > 0:
                third(j - 1, u)
    for u in range(CUTS):
        second(per - 1, u)
    for u in range(CUTS):
        third(per - 1, u)
    for j in range(per):
        third_in[j, z, q] = third_out[j, z, q]
    for j in range(per):
        others(lambda from_z, from_q: arrival(j, from_z, from_q).wait_recv(), 0, columns)
        for c in range(columns):
            total = third_in[j, 0, c].astype(jnp.float32)
            for k in range(1, depth):
                total = total + third_in[j, k, c].astype(jnp.float32)
            out_ref[:, c * per + j, :] = total
    for j in range(per):
        for u in range(CUTS):
            for h in range(2):
                for part in range(2):
                    stage_one(j, u, h, part).wait_send()
                stage_two(j, u, h).wait_send()
        others(lambda to_z, to_q: stage_three(j, to_z, to_q).wait_send(), 0, columns)
    ring(lambda to_g: post(to_g).wait_send())
    beside(lambda to_q: every(lambda from_g: hand(from_g, to_q).wait_send()))


def on_device(sources, owners, strip_rows, panel_counts, arrival_bins, arrival_fracs, gain_table):
    strips, terms, panels = sources.shape
    shards, columns = lax.axis_size("gx"), lax.axis_size("gy")
    cap = 2 * strips // shards
    rows, blocks = arrival_bins.shape[:2]
    observers = gain_table.shape[3]
    per = blocks // columns
    share = observers // (shards * columns)
    depth = shards // 4
    tall = depth * columns * share // CUTS
    half = NBIN // 2
    tiles_wide = observers // LANES
    wide = terms * panels + LANES
    assert panels == LANES and rows <= 256 and terms == 8
    flat = (
        gain_table.reshape(rows * terms, blocks, tiles_wide, LANES).transpose(0, 2, 1, 3).reshape(-1, LANES)
    )
    dma = pltpu.SemaphoreType.DMA
    return pl.pallas_call(
        functools.partial(signals_kernel, per, share, cap),
        out_shape=jax.ShapeDtypeStruct((share, blocks, NBIN), jnp.float32),
        in_specs=[pl.BlockSpec(memory_space=pltpu.VMEM)] * 4 + [pl.BlockSpec(memory_space=pl.ANY)] * 3,
        out_specs=pl.BlockSpec(memory_space=pltpu.VMEM),
        scratch_shapes=[
            pltpu.VMEM((per, observers, rows * terms), jnp.bfloat16),
            pltpu.VMEM((SLOTS, CHUNK * tiles_wide * blocks, LANES), jnp.bfloat16),
            pltpu.VMEM((per, CHUNK, observers), jnp.bfloat16),
            pltpu.VMEM((strips * terms, panels), jnp.float32),
            pltpu.VMEM((shards, cap, wide), jnp.bfloat16),
            pltpu.VMEM((columns, shards, cap, wide), jnp.bfloat16),
            pltpu.VMEM((rows * terms, panels), jnp.float32),
            pltpu.VMEM((rows * blocks, LANES), jnp.int32),
            pltpu.VMEM((rows * blocks, LANES), jnp.float32),
            pltpu.VMEM((rows * terms, NBIN), jnp.bfloat16),
            pltpu.VMEM((per, CUTS, 2, 2, tall, half), jnp.bfloat16),
            pltpu.VMEM((per, CUTS, 2, 2, tall, half), jnp.bfloat16),
            pltpu.VMEM((per, CUTS, 2, tall, half), jnp.float32),
            pltpu.VMEM((per, CUTS, 2, tall, half), jnp.float32),
            pltpu.VMEM((per, CUTS, 2, tall, half), jnp.bfloat16),
            pltpu.VMEM((per, CUTS, 2, tall, half), jnp.bfloat16),
            pltpu.VMEM((per, depth, columns, share, NBIN), jnp.bfloat16),
            pltpu.VMEM((per, depth, columns, share, NBIN), jnp.bfloat16),
            dma((SLOTS,)),
            dma((2,)),
            dma((shards,)),
            dma((shards,)),
            dma((columns, shards)),
            dma((columns, shards)),
            dma((per, CUTS, 2, 2)),
            dma((per, CUTS, 2, 2)),
            dma((per, CUTS, 2)),
            dma((per, CUTS, 2)),
            dma((per, depth, columns)),
            dma((per, depth, columns)),
        ],
        compiler_params=pltpu.CompilerParams(collective_id=0, has_side_effects=True),
        name="signals",
    )(
        sources,
        owners.reshape(1, strips),
        strip_rows.reshape(1, strips),
        panel_counts.reshape(1, strips),
        arrival_bins.reshape(-1, panels),
        arrival_fracs.reshape(-1, panels),
        flat,
    )


def solution(mesh):
    placed = (
        P(("gx", "gy"), None, None),
        P(("gx", "gy"), None),
        P(("gx", "gy")),
        P(("gx", "gy")),
        P("gx", None, None),
        P("gx", None, None),
        P("gx", None, None, None),
    )
    return jax.shard_map(
        on_device,
        mesh=mesh,
        in_specs=placed,
        out_specs=P(("gx", "gy"), None, None),
        check_vma=False,
    )
```
